32 devices in a mesh: ta: 4 (over z), gz: 4 (over x, core), gy: 2 (over y).
Axes of the slice: x: 2, y: 2, z: 4, core: 2. Of those that a mesh axis runs over, the one named last changes fastest.
Arguments:
- right_side: float32 [32, 32, 32, 128], P('ta', 'gz', 'gy'), may hold values from -12 to 12, as said below
- mass_field: float32 [32, 32, 32, 128], P('ta', 'gz', 'gy'), may hold values from 0.05 to 0.8
Outputs:
- solution: float32 [32, 32, 32, 128], P('ta', 'gz', 'gy')
- residual: float32 [32, 32, 32, 128], P('ta', 'gz', 'gy')
The draws below stay inside these ranges and needn't reach their ends.
Inputs may be any that keep to these rules, and one draw needn't show every extreme that they name: right_side is twice a field constant on aligned blocks of 8 x 8 x 8 x 8 sites plus site-by-site noise, each part within -4 to 4.
All inputs are finite; a program needn't handle non-finite values.
Results may differ from the reference program's by a relative error of at most 0.0003.
Values sent between devices are 32-bit elements.
A program may use at most 128 MiB of HBM per device.

```python
import math
import jax
import jax.numpy as jnp

LEVELS = 4
PRE = 2
POST = 2
COARSE_STEPS = 4
NT = 32
NZ = 32
NY = 32
NX = 128


def draw_right_side(key, part):
    coarse_key = jax.random.fold_in(key, 11)
    detail_key = jax.random.fold_in(key, 23)
    coarse_shape = (NT // 8, NZ // 8, NY // 8, NX // 8)
    whole_shape = (NT, NZ, NY, NX)
    coarse = jnp.clip(jax.random.normal(coarse_key, coarse_shape, jnp.float32), -4.0, 4.0)
    detail = jnp.clip(jax.random.normal(detail_key, whole_shape, jnp.float32), -4.0, 4.0)
    filled = coarse
    for dimension in range(4):
        filled = jnp.repeat(filled, 8, axis=dimension)
    return (2.0 * filled + detail).astype(jnp.float32)


def shard_levels(key, extent, shards, low, top_value):
    loudness = 1.0
    for position, blocks in shards:
        steps = jax.random.uniform(jax.random.fold_in(jax.random.fold_in(key, 6), position), (blocks,), jnp.float32, low / len(shards), top_value / len(shards))
        loudness = loudness * jnp.repeat(jnp.exp(steps), extent[position] // blocks).reshape((-1,) + (1,) * (len(extent) - 1 - position))
    return loudness


def setup_inputs(seed: int = 0) -> dict:
    keys = jax.random.split(jax.random.key(seed), 3)
    return {
        "right_side": draw_right_side(jax.random.fold_in(keys[2], 71), 0),
        "mass_field": jnp.clip(jnp.exp(math.log(0.8) - 2.7725887 * jax.random.uniform(keys[1], (NT, NZ, NY, NX), jnp.float32) ** shard_levels(keys[1], (NT, NZ, NY, NX), ((0, 4), (1, 4), (2, 2)), -0.2, 0.2)), 0.05, 0.8),
    }


DAMPING = 0.7


def neighbours(values):
    summed = jnp.zeros_like(values)
    for dimension in range(4):
        summed = summed + jnp.roll(values, 1, dimension) + jnp.roll(values, -1, dimension)
    return summed


def operate(values, mass_level, coarse_level):
    factor = 0.5 ** coarse_level
    return factor * (8.0 * values - neighbours(values)) + mass_level * values


def coarsen(values):
    first, second, third, fourth = values.shape
    blocks = values.reshape(first // 2, 2, second // 2, 2, third // 2, 2, fourth // 2, 2)
    return jnp.mean(blocks, axis=(1, 3, 5, 7))


def refine(values):
    for dimension in range(4):
        values = jnp.repeat(values, 2, axis=dimension)
    return values


def sweeps(values, source, mass_level, coarse_level, count_steps):
    diagonal = 8.0 * (0.5 ** coarse_level) + mass_level
    for sweep_no in range(count_steps):
        values = values + DAMPING * (source - operate(values, mass_level, coarse_level)) / diagonal
    return values


def cycle(source, mass_level, coarse_level):
    diagonal = 8.0 * (0.5 ** coarse_level) + mass_level
    values = DAMPING * source / diagonal
    if coarse_level == LEVELS - 1:
        return sweeps(values, source, mass_level, coarse_level, COARSE_STEPS - 1)
    values = sweeps(values, source, mass_level, coarse_level, PRE - 1)
    remainder = source - operate(values, mass_level, coarse_level)
    correction = cycle(coarsen(remainder), coarsen(mass_level), coarse_level + 1)
    values = values + refine(correction)
    return sweeps(values, source, mass_level, coarse_level, POST)


def reference(right_side, mass_field):
    solution = cycle(right_side, mass_field, 0)
    residual = right_side - operate(solution, mass_field, 0)
    return solution, residual
```

```python
import functools

import jax
import jax.numpy as jnp
from jax import lax
from jax.experimental import pallas as pl
from jax.experimental.pallas import tpu as pltpu
from jax.sharding import PartitionSpec as P

DAMPING = 0.7
KEEP = 1.0 - DAMPING
MESH = pl.DeviceIdType.MESH
ROUNDS = 8


def rolled(values, shift, axis):
    return pltpu.roll(values, shift % values.shape[axis], axis)


def pair_swap(values, step, axis):
    index = lax.broadcasted_iota(jnp.int32, values.shape, axis)
    return jnp.where((index // step) % 2 == 0, rolled(values, -step, axis), rolled(values, step, axis))


def coarsened(slabs, step):
    summed = slabs[0] + slabs[1]
    count, rows, lanes = summed.shape
    summed = summed.reshape(count // 2, 2, rows, lanes)
    summed = summed[:, 0] + summed[:, 1]
    summed = summed + pair_swap(summed, step, 1)
    return (summed + pair_swap(summed, step, 2)) * 0.0625


def refined_z(slab):
    return jnp.repeat(slab, 2, axis=0)


def shifted_z(slab, forward):
    if forward:
        return jnp.concatenate([slab[-1:], slab[:-1]], axis=0)
    return jnp.concatenate([slab[1:], slab[:1]], axis=0)


def kernel(sizes, s_ref, m_ref, sol_ref, res_ref, *scratch):
    nta, ngz, ngy = sizes
    (g0, v0a, v0b, v0w, v0x, v0s, y0, ys0,
     s1, m1, g1, v1a, v1b, v1w, v1x, v1s, y1, ys1,
     ms, mplane, mall, rs, rplane, rall, s2, m2, g2, u2, w2, e2, ey2,
     frsem, ffsem, gsend, grecv) = scratch
    size_t, size_z, rows, lanes = s_ref.shape
    ta, gz, gy = lax.axis_index("ta"), lax.axis_index("gz"), lax.axis_index("gy")

    plane = [(dz, dy) for dz in range(ngz) for dy in range(ngy) if dz or dy]
    line = list(range(1, nta))

    def plane_id(dz, dy):
        return {"gz": lax.rem(gz + dz, ngz), "gy": lax.rem(gy + dy, ngy)}

    def line_id(dt):
        return {"ta": lax.rem(ta + dt, nta)}

    barrier = pltpu.get_barrier_semaphore()
    for dz, dy in plane:
        pl.semaphore_signal(barrier, inc=1, device_id=plane_id(dz, dy), device_id_type=MESH)
    for dt in line:
        pl.semaphore_signal(barrier, inc=1, device_id=line_id(dt), device_id_type=MESH)

    def exchange(number, field, faces, halos):
        count_t, count_z = field.shape[0] - 2, field.shape[1] - 2
        inner_t, inner_z = pl.ds(1, count_t), pl.ds(1, count_z)
        up_t, down_t = {"ta": lax.rem(ta + 1, nta)}, {"ta": lax.rem(ta + nta - 1, nta)}
        up_z, down_z = {"gz": lax.rem(gz + 1, ngz)}, {"gz": lax.rem(gz + ngz - 1, ngz)}
        up_y, down_y = {"gy": lax.rem(gy + 1, ngy)}, {"gy": lax.rem(gy + ngy - 1, ngy)}
        moves = [
            (field.at[pl.ds(count_t, 1), inner_z], field.at[pl.ds(0, 1), inner_z], up_t),
            (field.at[pl.ds(1, 1), inner_z], field.at[pl.ds(count_t + 1, 1), inner_z], down_t),
            (field.at[inner_t, pl.ds(count_z, 1)], field.at[inner_t, pl.ds(0, 1)], up_z),
            (field.at[inner_t, pl.ds(1, 1)], field.at[inner_t, pl.ds(count_z + 1, 1)], down_z),
            (faces.at[1], halos.at[0], up_y),
            (faces.at[0], halos.at[1], down_y),
        ]
        copies = [
            pltpu.make_async_remote_copy(
                src_ref=source, dst_ref=target, send_sem=ffsem.at[number, place],
                recv_sem=frsem.at[number, place], device_id=device, device_id_type=MESH,
            )
            for place, (source, target, device) in enumerate(moves)
        ]
        for copy in copies:
            copy.start()

        def finish():
            for copy in copies:
                copy.wait()

        return finish

    def put(field, faces, t, slab):
        count_z = field.shape[1] - 2
        field[t + 1, pl.ds(1, count_z)] = slab
        faces[0, t] = slab[:, :1]
        faces[1, t] = slab[:, rows - 1:]

    def side_sum(field, halos, t, step):
        count_z = field.shape[1] - 2
        slab = field[t + 1, pl.ds(1, count_z)]
        row = lax.broadcasted_iota(jnp.int32, slab.shape, 1)
        summed = field[t, pl.ds(1, count_z)] + field[t + 2, pl.ds(1, count_z)]
        summed = summed + field[t + 1, pl.ds(0, count_z)] + field[t + 1, pl.ds(2, count_z)]
        summed = summed + jnp.where(row < step, halos[0, t], rolled(slab, step, 1))
        summed = summed + jnp.where(row >= rows - step, halos[1, t], rolled(slab, -step, 1))
        return slab, summed + rolled(slab, step, 2) + rolled(slab, -step, 2)

    def packed(out, field_slabs):
        index = lax.broadcasted_iota(jnp.int32, field_slabs[0].shape, 1)
        lane = lax.broadcasted_iota(jnp.int32, field_slabs[0].shape, 2)
        keep = index == 4 * (lane % 4)
        for t, slab in enumerate(field_slabs):
            count = slab.shape[0]
            row = jnp.sum(jnp.where(keep, slab, 0.0), axis=1, keepdims=True)
            out[pl.ds(t * count, count)] = row

    def plane_gather(first, source, target):
        copies = [
            pltpu.make_async_remote_copy(
                src_ref=source, dst_ref=target.at[gy, gz], send_sem=gsend.at[first + place],
                recv_sem=grecv.at[first + place], device_id=plane_id(dz, dy), device_id_type=MESH,
            )
            for place, (dz, dy) in enumerate(plane)
        ]
        for copy in copies:
            copy.start()
        target[gy, gz] = source[...]
        return copies

    def line_gather(first, source, target):
        copies = [
            pltpu.make_async_remote_copy(
                src_ref=source, dst_ref=target.at[ta], send_sem=gsend.at[first + place],
                recv_sem=grecv.at[first + place], device_id=line_id(dt), device_id_type=MESH,
            )
            for place, dt in enumerate(line)
        ]
        for copy in copies:
            copy.start()
        target[ta] = source[...]
        return copies

    def finish(copies):
        for copy in copies:
            copy.wait()

    rows2 = rows // 4
    all_t, all_z, all_y = 2 * nta, 2 * ngz, rows2 * ngy

    def unpacked(source, t):
        pair, odd = divmod(t, 2)
        count = size_z // 4
        shape = (all_z, all_y, lanes)
        row = lax.broadcasted_iota(jnp.int32, shape, 1)
        lane = lax.broadcasted_iota(jnp.int32, shape, 2)
        values = None
        for part in range(ngy):
            piece = source[pair, part, :, pl.ds(odd * count, count)].reshape(all_z, 1, lanes)
            piece = jnp.broadcast_to(piece, shape)
            values = piece if values is None else jnp.where(row >= part * rows2, piece, values)
        values = jnp.where(lane % 4 == row % rows2, values, 0.0)
        values = values + pair_swap(values, 1, 2)
        return values + pair_swap(values, 2, 2)

    for t in range(size_t):
        weight = DAMPING / (8.0 + m_ref[t])
        g0[t] = weight
        put(v0a, ys0.at[0], t, weight * s_ref[t])
    pl.semaphore_wait(barrier, len(plane) + len(line))
    done = exchange(0, v0a, ys0.at[0], y0.at[0])

    slabs = [coarsened((m_ref[2 * t], m_ref[2 * t + 1]), 1) for t in range(size_t // 2)]
    for t, slab in enumerate(slabs):
        m1[t] = slab
        g1[t] = DAMPING / (4.0 + slab)
    packed(ms, [coarsened((slabs[2 * t], slabs[2 * t + 1]), 2) for t in range(size_t // 4)])
    mass_copies = plane_gather(0, ms, mplane)
    done()

    for t in range(size_t):
        slab, summed = side_sum(v0a, y0.at[0], t, 1)
        put(v0b, ys0.at[1], t, KEEP * slab + g0[t] * (s_ref[t] + summed))
    done = exchange(1, v0b, ys0.at[1], y0.at[1])
    finish(mass_copies)
    mass_copies = line_gather(len(plane), mplane, mall)
    done()

    for t in range(size_t // 2):
        remainder = []
        for odd in range(2):
            slab, summed = side_sum(v0b, y0.at[1], 2 * t + odd, 1)
            remainder.append(s_ref[2 * t + odd] + summed - (8.0 + m_ref[2 * t + odd]) * slab)
        source = coarsened(remainder, 1)
        s1[t] = source
        put(v1a, ys1.at[0], t, g1[t] * source)
    done = exchange(2, v1a, ys1.at[0], y1.at[0])
    finish(mass_copies)
    for t in range(all_t):
        mass = unpacked(mall, t)
        m2[t] = mass
        g2[t] = DAMPING / (2.0 + mass)
    weights3 = []
    for t in range(all_t // 2):
        mass = coarse_full(m2[2 * t], m2[2 * t + 1])
        weights3.append(DAMPING / (1.0 + mass))
    done()

    for t in range(size_t // 2):
        slab, summed = side_sum(v1a, y1.at[0], t, 2)
        put(v1b, ys1.at[1], t, KEEP * slab + g1[t] * (s1[t] + 0.5 * summed))
    exchange(3, v1b, ys1.at[1], y1.at[1])()

    sources = []
    for t in range(size_t // 4):
        remainder = []
        for odd in range(2):
            slab, summed = side_sum(v1b, y1.at[1], 2 * t + odd, 2)
            remainder.append(s1[2 * t + odd] + 0.5 * summed - (4.0 + m1[2 * t + odd]) * slab)
        sources.append(coarsened(remainder, 2))
    packed(rs, sources)
    first = len(plane) + len(line)
    finish(plane_gather(first, rs, rplane))
    finish(line_gather(first + len(plane), rplane, rall))

    for t in range(all_t):
        source = unpacked(rall, t)
        s2[t] = source
        u2[t] = g2[t] * source

    def sum2(field, t):
        slab = field[t]
        summed = field[(t - 1) % all_t] + field[(t + 1) % all_t]
        summed = summed + shifted_z(slab, True) + shifted_z(slab, False)
        summed = summed + rolled(slab, 1, 1) + rolled(slab, -1, 1)
        return slab, summed + rolled(slab, 4, 2) + rolled(slab, -4, 2)

    def sweep2(field, out):
        for t in range(all_t):
            slab, summed = sum2(field, t)
            out[t] = KEEP * slab + g2[t] * (s2[t] + 0.25 * summed)

    sweep2(u2, w2)
    sources3 = []
    for t in range(all_t // 2):
        remainder = []
        for odd in range(2):
            slab, summed = sum2(w2, 2 * t + odd)
            remainder.append(s2[2 * t + odd] + 0.25 * summed - (2.0 + m2[2 * t + odd]) * slab)
        sources3.append(coarse_full(*remainder))

    values = [weight * source for weight, source in zip(weights3, sources3)]
    count = len(values)
    for sweep_no in range(3):
        fresh = []
        for t in range(count):
            slab = values[t]
            summed = values[(t - 1) % count] + values[(t + 1) % count]
            summed = summed + shifted_z(slab, True) + shifted_z(slab, False)
            summed = summed + rolled(slab, 2, 1) + rolled(slab, -2, 1)
            summed = summed + rolled(slab, 8, 2) + rolled(slab, -8, 2)
            fresh.append(KEEP * slab + weights3[t] * (sources3[t] + 0.125 * summed))
        values = fresh

    for t in range(all_t):
        w2[t] = w2[t] + refined_z(values[t // 2])
    sweep2(w2, u2)
    sweep2(u2, w2)

    part_t, part_z = size_t // 4, size_z // 4
    row = lax.broadcasted_iota(jnp.int32, (rows, lanes), 0)
    for a in range(part_t + 2):
        for b in range(part_z + 2):
            edge_t, edge_z = a in (0, part_t + 1), b in (0, part_z + 1)
            if edge_t and edge_z:
                continue
            at_t = lax.rem(ta * part_t + (a - 1 + all_t), all_t)
            at_z = lax.rem(gz * part_z + (b - 1 + all_z), all_z)

            def line_of(k):
                at_y = lax.rem(gy * rows2 + (k + all_y), all_y)
                return w2[at_t, at_z, pl.ds(at_y, 1)]

            slab = jnp.broadcast_to(line_of(0), (rows, lanes))
            for k in range(1, rows2):
                slab = jnp.where(row >= 4 * k, line_of(k), slab)
            e2[a, b] = slab
            if not (edge_t or edge_z):
                ey2[0, a - 1, b - 1] = line_of(-1)
                ey2[1, a - 1, b - 1] = line_of(rows2)

    def corrected(out, field, halos, out_halos, coarse, coarse_halos):
        count_t, count_z = field.shape[0] - 2, field.shape[1] - 2
        inner = pl.ds(1, count_z)
        inner_coarse = pl.ds(1, count_z // 2)
        for p in range(count_t + 2):
            out[p, inner] = field[p, inner] + refined_z(coarse[(p + 1) // 2, inner_coarse])
        for p in range(1, count_t + 1):
            for q in (0, count_z + 1):
                out[p, q] = field[p, q] + coarse[(p + 1) // 2, (q + 1) // 2]
        for side in range(2):
            for t in range(count_t):
                out_halos[side, t] = halos[side, t] + refined_z(coarse_halos[side, t // 2])

    corrected(v1w, v1b, y1.at[1], y1.at[2], e2, ey2)
    for t in range(size_t // 2):
        slab, summed = side_sum(v1w, y1.at[2], t, 2)
        put(v1x, ys1.at[2], t, KEEP * slab + g1[t] * (s1[t] + 0.5 * summed))
    exchange(4, v1x, ys1.at[2], y1.at[3])()
    for t in range(size_t // 2):
        slab, summed = side_sum(v1x, y1.at[3], t, 2)
        put(v1s, ys1.at[3], t, KEEP * slab + g1[t] * (s1[t] + 0.5 * summed))
    exchange(5, v1s, ys1.at[3], y1.at[4])()

    corrected(v0w, v0b, y0.at[1], y0.at[2], v1s, y1.at[4])
    for t in range(size_t):
        slab, summed = side_sum(v0w, y0.at[2], t, 1)
        put(v0x, ys0.at[2], t, KEEP * slab + g0[t] * (s_ref[t] + summed))
    exchange(6, v0x, ys0.at[2], y0.at[3])()
    for t in range(size_t):
        slab, summed = side_sum(v0x, y0.at[3], t, 1)
        fresh = KEEP * slab + g0[t] * (s_ref[t] + summed)
        put(v0s, ys0.at[3], t, fresh)
        sol_ref[t] = fresh
    exchange(7, v0s, ys0.at[3], y0.at[4])()
    for t in range(size_t):
        slab, summed = side_sum(v0s, y0.at[4], t, 1)
        res_ref[t] = s_ref[t] + summed - (8.0 + m_ref[t]) * slab


def coarse_full(even, odd):
    summed = even + odd
    count, rows, lanes = summed.shape
    summed = summed.reshape(count // 2, 2, rows, lanes)
    summed = summed[:, 0] + summed[:, 1]
    summed = summed + pair_swap(summed, 1, 1)
    return (summed + pair_swap(summed, 4, 2)) * 0.0625


def per_device(sizes, right_side, mass_field):
    nta, ngz, ngy = sizes
    size_t, size_z, rows, lanes = right_side.shape
    half_t, half_z = size_t // 2, size_z // 2
    part_t, part_z, rows2 = size_t // 4, size_z // 4, rows // 4
    peers = ngz * ngy - 1 + nta - 1
    vmem = lambda *shape: pltpu.VMEM(shape, jnp.float32)
    padded0 = vmem(size_t + 2, size_z + 2, rows, lanes)
    padded1 = vmem(half_t + 2, half_z + 2, rows, lanes)
    whole2 = vmem(part_t * nta, part_z * ngz, rows2 * ngy, lanes)
    packs = [
        vmem(part_t * part_z, 1, lanes),
        vmem(ngy, ngz, part_t * part_z, 1, lanes),
        vmem(nta, ngy, ngz, part_t * part_z, 1, lanes),
    ]
    scratch = [
        vmem(size_t, size_z, rows, lanes), padded0, padded0, padded0, padded0, padded0,
        vmem(5, 2, size_t, size_z, 1, lanes), vmem(4, 2, size_t, size_z, 1, lanes),
        vmem(half_t, half_z, rows, lanes), vmem(half_t, half_z, rows, lanes),
        vmem(half_t, half_z, rows, lanes), padded1, padded1, padded1, padded1, padded1,
        vmem(5, 2, half_t, half_z, 1, lanes), vmem(4, 2, half_t, half_z, 1, lanes),
        *packs, *packs, whole2, whole2, whole2, whole2, whole2,
        vmem(part_t + 2, part_z + 2, rows, lanes), vmem(2, part_t, part_z, 1, lanes),
        pltpu.SemaphoreType.DMA((ROUNDS, 6)), pltpu.SemaphoreType.DMA((ROUNDS, 6)),
        pltpu.SemaphoreType.DMA((2 * peers,)), pltpu.SemaphoreType.DMA((2 * peers,)),
    ]
    block = jax.ShapeDtypeStruct(right_side.shape, jnp.float32)
    return pl.pallas_call(
        functools.partial(kernel, sizes),
        out_shape=(block, block),
        in_specs=[pl.BlockSpec(memory_space=pltpu.VMEM)] * 2,
        out_specs=(pl.BlockSpec(memory_space=pltpu.VMEM),) * 2,
        scratch_shapes=scratch,
        compiler_params=pltpu.CompilerParams(
            collective_id=0, has_side_effects=True, vmem_limit_bytes=48 * 1024 * 1024
        ),
    )(right_side, mass_field)


def solution(mesh):
    sizes = tuple(mesh.shape[axis] for axis in ("ta", "gz", "gy"))
    spec = P("ta", "gz", "gy", None)
    return jax.shard_map(
        functools.partial(per_device, sizes),
        mesh=mesh,
        in_specs=(spec, spec),
        out_specs=(spec, spec),
        check_vma=False,
    )
```

```python
import functools

import jax
import jax.numpy as jnp
from jax import lax
from jax.experimental import pallas as pl
from jax.experimental.pallas import tpu as pltpu
from jax.sharding import PartitionSpec as P

DAMPING = 0.7
KEEP = 1.0 - DAMPING
MESH = pl.DeviceIdType.MESH


def rolled(values, shift, axis):
    return pltpu.roll(values, shift % values.shape[axis], axis)


def pair_swap(values, step, axis):
    index = lax.broadcasted_iota(jnp.int32, values.shape, axis)
    return jnp.where((index // step) % 2 == 0, rolled(values, -step, axis), rolled(values, step, axis))


def z_pairs(summed):
    count, rows, lanes = summed.shape
    summed = summed.reshape(count // 2, 2, rows, lanes)
    return summed[:, 0] + summed[:, 1]


def refined_z(slab):
    return jnp.repeat(slab, 2, axis=0)


def shifted_z(slab, forward):
    if forward:
        return jnp.concatenate([slab[-1:], slab[:-1]], axis=0)
    return jnp.concatenate([slab[1:], slab[:1]], axis=0)


def kernel(sizes, s_ref, m_ref, sol_ref, res_ref, *scratch):
    nta, ngz, ngy = sizes
    (g0, v0a, v0b, v0w, v0x, v0s, y0, ys0, fold,
     s1, m1, g1, v1a, v1b, v1w, v1x, e1, e2,
     mall, rall, s2, m2, g2, u2, w2,
     f0s, f0r, f1s, f1r, fxs, fxr, gsend, grecv) = scratch
    size_t, size_z, rows, lanes = s_ref.shape
    size_t1, size_z1, rows1 = size_t // 2, size_z // 2, rows // 2
    part_t, part_z, rows2 = size_t // 4, size_z // 4, rows // 4
    all_t, all_z = part_t * nta, part_z * ngz
    ta, gz, gy = lax.axis_index("ta"), lax.axis_index("gz"), lax.axis_index("gy")

    def device(dt, dz, dy):
        return {
            "ta": lax.rem(ta + dt + nta, nta),
            "gz": lax.rem(gz + dz + ngz, ngz),
            "gy": lax.rem(gy + dy + ngy, ngy),
        }

    near = [(dt, dz, dy) for dt in (-1, 0, 1) for dz in (-1, 0, 1) for dy in range(ngy)]
    across = [(dt, dz, 0) for dt in range(nta) for dz in range(ngz) if dt or dz]
    met = sorted({(dt % nta, dz % ngz, dy % ngy) for dt, dz, dy in near + across} - {(0, 0, 0)})
    barrier = pltpu.get_barrier_semaphore()
    for offset in met:
        pl.semaphore_signal(barrier, inc=1, device_id=device(*offset), device_id_type=MESH)

    def send(moves, sends, receives):
        copies = [
            pltpu.make_async_remote_copy(
                src_ref=source, dst_ref=target, send_sem=sends(place), recv_sem=receives(place),
                device_id=device(*offset), device_id_type=MESH,
            )
            for place, (source, target, offset) in enumerate(moves)
        ]
        for copy in copies:
            copy.start()
        return copies

    def finish(copies):
        for copy in copies:
            copy.wait()

    def exchange0(number, field, faces, halos):
        inner_t, inner_z = pl.ds(1, size_t), pl.ds(1, size_z)
        moves = [
            (field.at[pl.ds(size_t, 1), inner_z], field.at[pl.ds(0, 1), inner_z], (1, 0, 0)),
            (field.at[pl.ds(1, 1), inner_z], field.at[pl.ds(size_t + 1, 1), inner_z], (-1, 0, 0)),
            (field.at[inner_t, pl.ds(size_z, 1)], field.at[inner_t, pl.ds(0, 1)], (0, 1, 0)),
            (field.at[inner_t, pl.ds(1, 1)], field.at[inner_t, pl.ds(size_z + 1, 1)], (0, -1, 0)),
            (faces.at[1], halos.at[0], (0, 0, 1)),
            (faces.at[0], halos.at[1], (0, 0, -1)),
        ]
        copies = send(moves, lambda place: f0s.at[number, place], lambda place: f0r.at[number, place])
        return copies[:2], copies[2:]

    def around(field, part, dy):
        own_t, own_z = pl.ds(2, size_t1), pl.ds(2, size_z1)
        spans = {
            1: (lambda size, deep: (pl.ds(2 + size - deep, deep), pl.ds(2 - deep, deep))),
            -1: (lambda size, deep: (pl.ds(2, deep), pl.ds(2 + size, deep))),
        }
        moves = []
        for step in (1, -1):
            here, there = spans[step](size_t1, 2)
            moves.append((field.at[(here, own_z) + part], field.at[(there, own_z) + part], (step, 0, dy)))
            here, there = spans[step](size_z1, 2)
            moves.append((field.at[(own_t, here) + part], field.at[(own_t, there) + part], (0, step, dy)))
        for step_t in (1, -1):
            for step_z in (1, -1):
                here_t, there_t = spans[step_t](size_t1, 1)
                here_z, there_z = spans[step_z](size_z1, 1)
                moves.append((
                    field.at[(here_t, here_z) + part], field.at[(there_t, there_z) + part],
                    (step_t, step_z, dy),
                ))
        return moves

    def spread1(number, field):
        moves = []
        own = field.at[pl.ds(2, size_t1), pl.ds(2, size_z1), pl.ds(gy, 1)]
        for dy in range(ngy):
            moves += around(field, (pl.ds(gy, 1),), dy)
        moves += [(own, own, (0, 0, dy)) for dy in range(1, ngy)]
        return send(moves, lambda place: f1s.at[number, place], lambda place: f1r.at[number, place])

    def gather(number, field):
        own = field.at[ta, gz]
        return send(
            [(own, own, offset) for offset in across],
            lambda place: gsend.at[number, place], lambda place: grecv.at[number, place],
        )

    def put(field, faces, t, slab):
        field[t + 1, pl.ds(1, size_z)] = slab
        faces[0, t] = slab[:, :1]
        faces[1, t] = slab[:, rows - 1:]

    def sum0(field, halos, t):
        slab = field[t + 1, pl.ds(1, size_z)]
        row = lax.broadcasted_iota(jnp.int32, slab.shape, 1)
        summed = field[t, pl.ds(1, size_z)] + field[t + 2, pl.ds(1, size_z)]
        summed = summed + field[t + 1, pl.ds(0, size_z)] + field[t + 1, pl.ds(2, size_z)]
        summed = summed + jnp.where(row == 0, halos[0, t], rolled(slab, 1, 1))
        summed = summed + jnp.where(row == rows - 1, halos[1, t], rolled(slab, -1, 1))
        return slab, summed + rolled(slab, 1, 2) + rolled(slab, -1, 2)

    def halved(summed, place, step):
        count, high, _ = summed.shape
        view = fold.at[place, pl.ds(0, count)]
        view[...] = summed
        summed = view[:, pl.ds(0, high // 2, stride=2), :] + view[:, pl.ds(1, high // 2, stride=2), :]
        return (summed + pair_swap(summed, step, 2)) * 0.0625

    def doubled(slab, place):
        count, high, _ = slab.shape
        view = fold.at[place, pl.ds(0, count)]
        view[:, pl.ds(0, high, stride=2), :] = slab
        view[:, pl.ds(1, high, stride=2), :] = slab
        return view[...]

    full = ngy * rows1

    def near1(radius):
        for a in range(2 - radius, 2 + size_t1 + radius):
            reach = radius - max(2 - a, a - 1 - size_t1, 0)
            yield a, 2 - reach, size_z1 + 2 * reach

    def read1(field, a, b, count):
        return field[a, pl.ds(b, count)].reshape(count, full, lanes)

    def write1(field, a, b, slab):
        field[a, pl.ds(b, slab.shape[0])] = slab.reshape(slab.shape[0], ngy, rows1, lanes)

    def sum1(field, a, b, count):
        slab = read1(field, a, b, count)
        summed = read1(field, a - 1, b, count) + read1(field, a + 1, b, count)
        summed = summed + read1(field, a, b - 1, count) + read1(field, a, b + 1, count)
        summed = summed + rolled(slab, 1, 1) + rolled(slab, -1, 1)
        return slab, summed + rolled(slab, 2, 2) + rolled(slab, -2, 2)

    def sweep1(field, out, radius):
        for a, b, count in near1(radius):
            slab, summed = sum1(field, a, b, count)
            fresh = KEEP * slab + read1(g1, a, b, count) * (read1(s1, a, b, count) + 0.5 * summed)
            write1(out, a, b, fresh)

    def packed(out, slabs):
        parts = [slab[z] for slab in slabs for z in range(part_z)]
        lane = lax.broadcasted_iota(jnp.int32, parts[0].shape, 1)
        values = parts[0]
        for k in range(1, len(parts)):
            values = jnp.where(lane % 4 == k, parts[k], values)
        out[ta, gz] = values

    def unpacked(source, t):
        pair, odd = divmod(t, part_t)
        values = source[pair]
        lane = lax.broadcasted_iota(jnp.int32, values.shape, 2)
        pieces = []
        for z in range(part_z):
            piece = jnp.where(lane % 4 == odd * part_z + z, values, 0.0)
            piece = piece + pair_swap(piece, 1, 2)
            pieces.append(piece + pair_swap(piece, 2, 2))
        return jnp.stack(pieces, axis=1).reshape(all_z, ngy * rows2, lanes)

    inside = list(range(1, size_t - 1))
    ends = [0, size_t - 1]

    for t in range(size_t):
        weight = DAMPING / (8.0 + m_ref[t])
        g0[t] = weight
        put(v0a, ys0.at[0], t, weight * s_ref[t])
    pl.semaphore_wait(barrier, len(met))
    over_t, sides = exchange0(0, v0a, ys0.at[0], y0.at[0])
    for t in range(size_t1):
        mean = halved(z_pairs(m_ref[2 * t] + m_ref[2 * t + 1]), t, 1)
        m1[t + 2, pl.ds(2, size_z1), gy] = mean
    mass_copies = spread1(0, m1)

    def sweep0(field, halos, out, faces, ts, also=None):
        for t in ts:
            slab, summed = sum0(field, halos, t)
            fresh = KEEP * slab + g0[t] * (s_ref[t] + summed)
            put(out, faces, t, fresh)
            if also is not None:
                also[t] = fresh

    finish(sides)
    sweep0(v0a, y0.at[0], v0b, ys0.at[1], inside)
    finish(over_t)
    sweep0(v0a, y0.at[0], v0b, ys0.at[1], ends)
    over_t, sides = exchange0(1, v0b, ys0.at[1], y0.at[1])
    finish(mass_copies)
    for a, b, count in near1(2):
        write1(g1, a, b, DAMPING / (4.0 + read1(m1, a, b, count)))

    def to_level2(slabs):
        return [
            halved(z_pairs(slabs[2 * t] + slabs[2 * t + 1]), t, 2) for t in range(part_t)
        ]

    packed(mall, to_level2([read1(m1, 2 + t, 2, size_z1) for t in range(size_t1)]))
    mass_copies = gather(0, mall)

    def remainder0(ts):
        for t in ts:
            remainder = []
            for odd in range(2):
                slab, summed = sum0(v0b, y0.at[1], 2 * t + odd)
                remainder.append(s_ref[2 * t + odd] + summed - (8.0 + m_ref[2 * t + odd]) * slab)
            s1[t + 2, pl.ds(2, size_z1), gy] = halved(z_pairs(remainder[0] + remainder[1]), t, 1)

    finish(sides)
    remainder0(range(1, size_t1 - 1))
    finish(over_t)
    remainder0((0, size_t1 - 1))
    source_copies = spread1(1, s1)
    finish(mass_copies)
    for t in range(all_t):
        mass = unpacked(mall, t)
        m2[t] = mass
        g2[t] = DAMPING / (2.0 + mass)
    weights3 = [
        DAMPING / (1.0 + coarse_full(m2[2 * t], m2[2 * t + 1])) for t in range(all_t // 2)
    ]
    finish(source_copies)

    for a, b, count in near1(2):
        write1(v1a, a, b, read1(g1, a, b, count) * read1(s1, a, b, count))
    sweep1(v1a, v1b, 1)
    remainder = []
    for a, b, count in near1(0):
        slab, summed = sum1(v1b, a, b, count)
        remainder.append(
            read1(s1, a, b, count) + 0.5 * summed - (4.0 + read1(m1, a, b, count)) * slab
        )
    packed(rall, to_level2(remainder))
    finish(gather(1, rall))

    for t in range(all_t):
        source = unpacked(rall, t)
        s2[t] = source
        u2[t] = g2[t] * source

    def sum2(field, t):
        slab = field[t]
        summed = field[(t - 1) % all_t] + field[(t + 1) % all_t]
        summed = summed + shifted_z(slab, True) + shifted_z(slab, False)
        summed = summed + rolled(slab, 1, 1) + rolled(slab, -1, 1)
        return slab, summed + rolled(slab, 4, 2) + rolled(slab, -4, 2)

    def sweep2(field, out):
        for t in range(all_t):
            slab, summed = sum2(field, t)
            out[t] = KEEP * slab + g2[t] * (s2[t] + 0.25 * summed)

    sweep2(u2, w2)
    sources3 = []
    for t in range(all_t // 2):
        remainder = []
        for odd in range(2):
            slab, summed = sum2(w2, 2 * t + odd)
            remainder.append(s2[2 * t + odd] + 0.25 * summed - (2.0 + m2[2 * t + odd]) * slab)
        sources3.append(coarse_full(*remainder))

    values = [weight * source for weight, source in zip(weights3, sources3)]
    count = len(values)
    for sweep_no in range(3):
        fresh = []
        for t in range(count):
            slab = values[t]
            summed = values[(t - 1) % count] + values[(t + 1) % count]
            summed = summed + shifted_z(slab, True) + shifted_z(slab, False)
            summed = summed + rolled(slab, 2, 1) + rolled(slab, -2, 1)
            summed = summed + rolled(slab, 8, 2) + rolled(slab, -8, 2)
            fresh.append(KEEP * slab + weights3[t] * (sources3[t] + 0.125 * summed))
        values = fresh

    for t in range(all_t):
        w2[t] = w2[t] + refined_z(values[t // 2])
    sweep2(w2, u2)
    sweep2(u2, w2)

    for a in range(part_t + 2):
        at_t = lax.rem(ta * part_t + (a - 1 + all_t), all_t)
        slabs = []
        for b in range(part_z + 2):
            at_z = lax.rem(gz * part_z + (b - 1 + all_z), all_z)
            slabs.append(w2[at_t, pl.ds(at_z, 1)])
        e2[a] = doubled(jnp.concatenate(slabs, axis=0), a)
    for a, b, count in near1(1):
        fine = refined_z(e2[a // 2])
        write1(v1w, a, b, read1(v1b, a, b, count) + fine[b:b + count])
    sweep1(v1w, v1x, 0)
    finish(send(
        around(v1x, (), 0), lambda place: fxs.at[place], lambda place: fxr.at[place],
    ))
    sweep1(v1x, e1, 1)

    under = lax.rem(gy + ngy - 1, ngy)
    over = lax.rem(gy + 1, ngy)
    for p in range(size_t + 2):
        at_t = (p + 1) // 2 + 1
        if p in (0, size_t + 1):
            fine = refined_z(doubled(e1[at_t, pl.ds(2, size_z1), gy], 0))
            v0w[p, pl.ds(1, size_z)] = v0b[p, pl.ds(1, size_z)] + fine
        else:
            if p % 2:
                fine = refined_z(doubled(e1[at_t, pl.ds(1, size_z1 + 2), gy], p // 2 % 4))
                fine = fine[1:1 + size_z + 2]
                low = refined_z(e1[at_t, pl.ds(2, size_z1), under, pl.ds(rows1 - 1, 1)])
                high = refined_z(e1[at_t, pl.ds(2, size_z1), over, pl.ds(0, 1)])
            v0w[p] = v0b[p] + fine
            y0[2, 0, p - 1] = y0[1, 0, p - 1] + low
            y0[2, 1, p - 1] = y0[1, 1, p - 1] + high
    sweep0(v0w, y0.at[2], v0x, ys0.at[2], ends + inside)
    over_t, sides = exchange0(2, v0x, ys0.at[2], y0.at[3])
    finish(sides)
    sweep0(v0x, y0.at[3], v0s, ys0.at[3], inside, sol_ref)
    finish(over_t)
    sweep0(v0x, y0.at[3], v0s, ys0.at[3], ends, sol_ref)
    over_t, sides = exchange0(3, v0s, ys0.at[3], y0.at[4])

    def residual(ts):
        for t in ts:
            slab, summed = sum0(v0s, y0.at[4], t)
            res_ref[t] = s_ref[t] + summed - (8.0 + m_ref[t]) * slab

    finish(sides)
    residual(inside)
    finish(over_t)
    residual(ends)


def coarse_full(even, odd):
    summed = even + odd
    count, rows, lanes = summed.shape
    summed = summed.reshape(count // 2, 2, rows, lanes)
    summed = summed[:, 0] + summed[:, 1]
    summed = summed + pair_swap(summed, 1, 1)
    return (summed + pair_swap(summed, 4, 2)) * 0.0625


def per_device(sizes, right_side, mass_field):
    nta, ngz, ngy = sizes
    size_t, size_z, rows, lanes = right_side.shape
    size_t1, size_z1, rows1 = size_t // 2, size_z // 2, rows // 2
    part_t, part_z, rows2 = size_t // 4, size_z // 4, rows // 4
    vmem = lambda *shape: pltpu.VMEM(shape, jnp.float32)
    dma = lambda *shape: pltpu.SemaphoreType.DMA(shape)
    padded0 = vmem(size_t + 2, size_z + 2, rows, lanes)
    padded1 = vmem(size_t1 + 4, size_z1 + 4, ngy, rows1, lanes)
    whole2 = vmem(part_t * nta, part_z * ngz, rows2 * ngy, lanes)
    packs = vmem(nta, ngz, rows2 * ngy, lanes)
    spreads, peers = 8 * ngy + ngy - 1, nta * ngz - 1
    scratch = [
        vmem(size_t, size_z, rows, lanes), padded0, padded0, padded0, padded0, padded0,
        vmem(5, 2, size_t, size_z, 1, lanes), vmem(4, 2, size_t, size_z, 1, lanes),
        vmem(max(size_t1, part_t + 2), size_z, max(rows, ngy * rows1), lanes),
        *[padded1] * 8, vmem(part_t + 2, part_z + 2, ngy * rows1, lanes),
        packs, packs, *[whole2] * 5,
        dma(4, 6), dma(4, 6), dma(2, spreads), dma(2, spreads), dma(8), dma(8),
        dma(2, peers), dma(2, peers),
    ]
    block = jax.ShapeDtypeStruct(right_side.shape, jnp.float32)
    return pl.pallas_call(
        functools.partial(kernel, sizes),
        out_shape=(block, block),
        in_specs=[pl.BlockSpec(memory_space=pltpu.VMEM)] * 2,
        out_specs=(pl.BlockSpec(memory_space=pltpu.VMEM),) * 2,
        scratch_shapes=scratch,
        compiler_params=pltpu.CompilerParams(
            collective_id=0, has_side_effects=True, vmem_limit_bytes=48 * 1024 * 1024
        ),
    )(right_side, mass_field)


def solution(mesh):
    sizes = tuple(mesh.shape[axis] for axis in ("ta", "gz", "gy"))
    spec = P("ta", "gz", "gy", None)
    return jax.shard_map(
        functools.partial(per_device, sizes),
        mesh=mesh,
        in_specs=(spec, spec),
        out_specs=(spec, spec),
        check_vma=False,
    )
```

```python
import functools

import jax
import jax.numpy as jnp
from jax import lax
from jax.experimental import pallas as pl
from jax.experimental.pallas import tpu as pltpu
from jax.sharding import PartitionSpec as P

DAMPING = 0.7
KEEP = 1.0 - DAMPING
MESH = pl.DeviceIdType.MESH


def rolled(values, shift, axis):
    return pltpu.roll(values, shift % values.shape[axis], axis)


def pair_swap(values, step, axis):
    index = lax.broadcasted_iota(jnp.int32, values.shape, axis)
    return jnp.where((index // step) % 2 == 0, rolled(values, -step, axis), rolled(values, step, axis))


def z_pairs(summed):
    count, rows, lanes = summed.shape
    summed = summed.reshape(count // 2, 2, rows, lanes)
    return summed[:, 0] + summed[:, 1]


def refined_z(slab):
    return jnp.repeat(slab, 2, axis=0)


def shifted_z(slab, forward):
    if forward:
        return jnp.concatenate([slab[-1:], slab[:-1]], axis=0)
    return jnp.concatenate([slab[1:], slab[:1]], axis=0)


def kernel(sizes, s_hbm, m_hbm, sol_ref, res_ref, *scratch):
    nta, ngz, ngy = sizes
    (g0, v0a, v0b, v0w, v0x, v0s, y0, ys0, fold,
     s1, m1, g1, v1a, v1b, v1w, v1x, e1, e2,
     mall, rall, s2, m2, g2, u2, w2,
     f0s, f0r, f1s, f1r, fxs, fxr, gsend, grecv, s_ref, m_ref, loaded) = scratch
    size_t, size_z, rows, lanes = s_ref.shape
    size_t1, size_z1, rows1 = size_t // 2, size_z // 2, rows // 2
    part_t, part_z, rows2 = size_t // 4, size_z // 4, rows // 4
    all_t, all_z = part_t * nta, part_z * ngz
    ta, gz, gy = lax.axis_index("ta"), lax.axis_index("gz"), lax.axis_index("gy")

    first_up = lax.min(ta, 1)

    def device(dt, dz, dy):
        return {
            "ta": lax.rem(ta + dt + nta, nta),
            "gz": lax.rem(gz + dz + ngz, ngz),
            "gy": lax.rem(gy + dy + ngy, ngy),
        }

    near = [(dt, dz, dy) for dt in (-1, 0, 1) for dz in (-1, 0, 1) for dy in range(ngy)]
    across = [(dt, dz, 0) for dt in reversed(range(nta)) for dz in range(ngz) if dt or dz]
    loads = []
    for t in range(size_t):
        loads.append((
            pltpu.make_async_copy(m_hbm.at[pl.ds(t, 1)], m_ref.at[pl.ds(t, 1)], loaded.at[0, t]),
            pltpu.make_async_copy(s_hbm.at[pl.ds(t, 1)], s_ref.at[pl.ds(t, 1)], loaded.at[1, t]),
        ))
    met = sorted({(dt % nta, dz % ngz, dy % ngy) for dt, dz, dy in near + across} - {(0, 0, 0)})
    barrier = pltpu.get_barrier_semaphore()
    for offset in met:
        pl.semaphore_signal(barrier, inc=1, device_id=device(*offset), device_id_type=MESH)
    for pair in loads:
        for load in pair:
            load.start()

    def send(moves, sends, receives):
        copies = [
            pltpu.make_async_remote_copy(
                src_ref=source, dst_ref=target, send_sem=sends(place), recv_sem=receives(place),
                device_id=device(*offset), device_id_type=MESH,
            )
            for place, source, target, offset in moves
        ]
        for copy in copies:
            copy.start()
        return copies

    def finish(copies):
        for copy in copies:
            copy.wait()

    def exchange0(number, field, faces, halos):
        inner_t, inner_z = pl.ds(1, size_t), pl.ds(1, size_z)
        moves = []
        for up in (first_up, 1 - first_up):
            here, there = pl.ds(1 + (size_t - 1) * up, 1), pl.ds((size_t + 1) * (1 - up), 1)
            moves.append((up, field.at[here, inner_z], field.at[there, inner_z], (2 * up - 1, 0, 0)))
        moves += [
            (2, field.at[inner_t, pl.ds(size_z, 1)], field.at[inner_t, pl.ds(0, 1)], (0, 1, 0)),
            (3, field.at[inner_t, pl.ds(1, 1)], field.at[inner_t, pl.ds(size_z + 1, 1)], (0, -1, 0)),
            (4, faces.at[1], halos.at[0], (0, 0, 1)),
            (5, faces.at[0], halos.at[1], (0, 0, -1)),
        ]
        copies = send(moves, lambda place: f0s.at[number, place], lambda place: f0r.at[number, place])
        return copies[:2], copies[2:]

    def around(field, part, dys):
        own_t, own_z = pl.ds(2, size_t1), pl.ds(2, size_z1)

        def span(size, deep, up):
            return pl.ds(2 + (size - deep) * up, deep), pl.ds(2 + size - (size + deep) * up, deep)

        moves = []
        for up in (first_up, 1 - first_up):
            here, there = span(size_t1, 2, up)
            for dy in dys:
                moves.append((
                    8 * dy + up, field.at[(here, own_z) + part], field.at[(there, own_z) + part],
                    (2 * up - 1, 0, dy),
                ))
        for up in (1, 0):
            here_t, there_t = span(size_t1, 1, up)
            for up_z in (1, 0):
                here_z, there_z = span(size_z1, 1, up_z)
                for dy in dys:
                    moves.append((
                        8 * dy + 2 + 2 * up + up_z,
                        field.at[(here_t, here_z) + part], field.at[(there_t, there_z) + part],
                        (2 * up - 1, 2 * up_z - 1, dy),
                    ))
        for up in (1, 0):
            here, there = span(size_z1, 2, up)
            for dy in dys:
                moves.append((
                    8 * dy + 6 + up, field.at[(own_t, here) + part], field.at[(own_t, there) + part],
                    (0, 2 * up - 1, dy),
                ))
        return moves

    def spread1(number, field):
        own = field.at[pl.ds(2, size_t1), pl.ds(2, size_z1), pl.ds(gy, 1)]
        moves = around(field, (pl.ds(gy, 1),), range(ngy))
        moves += [(8 * ngy + dy - 1, own, own, (0, 0, dy)) for dy in range(1, ngy)]
        return send(moves, lambda place: f1s.at[number, place], lambda place: f1r.at[number, place])

    def gather(number, field):
        own = field.at[ta, gz]
        return send(
            [(place, own, own, offset) for place, offset in enumerate(across)],
            lambda place: gsend.at[number, place], lambda place: grecv.at[number, place],
        )

    def put(field, faces, t, slab):
        field[t + 1, pl.ds(1, size_z)] = slab
        faces[0, t] = slab[:, :1]
        faces[1, t] = slab[:, rows - 1:]

    def sum0(field, halos, t):
        slab = field[t + 1, pl.ds(1, size_z)]
        row = lax.broadcasted_iota(jnp.int32, slab.shape, 1)
        summed = field[t, pl.ds(1, size_z)] + field[t + 2, pl.ds(1, size_z)]
        summed = summed + field[t + 1, pl.ds(0, size_z)] + field[t + 1, pl.ds(2, size_z)]
        summed = summed + jnp.where(row == 0, halos[0, t], rolled(slab, 1, 1))
        summed = summed + jnp.where(row == rows - 1, halos[1, t], rolled(slab, -1, 1))
        return slab, summed + rolled(slab, 1, 2) + rolled(slab, -1, 2)

    def halved(summed, place, step):
        count, high, _ = summed.shape
        view = fold.at[place, pl.ds(0, count)]
        view[...] = summed
        summed = view[:, pl.ds(0, high // 2, stride=2), :] + view[:, pl.ds(1, high // 2, stride=2), :]
        return (summed + pair_swap(summed, step, 2)) * 0.0625

    def doubled(slab, place):
        count, high, _ = slab.shape
        view = fold.at[place, pl.ds(0, count)]
        view[:, pl.ds(0, high, stride=2), :] = slab
        view[:, pl.ds(1, high, stride=2), :] = slab
        return view[...]

    full = ngy * rows1

    def near1(radius):
        for a in range(2 - radius, 2 + size_t1 + radius):
            reach = radius - max(2 - a, a - 1 - size_t1, 0)
            yield a, 2 - reach, size_z1 + 2 * reach

    def read1(field, a, b, count):
        return field[a, pl.ds(b, count)].reshape(count, full, lanes)

    def write1(field, a, b, slab):
        field[a, pl.ds(b, slab.shape[0])] = slab.reshape(slab.shape[0], ngy, rows1, lanes)

    def sum1(field, a, b, count):
        slab = read1(field, a, b, count)
        summed = read1(field, a - 1, b, count) + read1(field, a + 1, b, count)
        summed = summed + read1(field, a, b - 1, count) + read1(field, a, b + 1, count)
        summed = summed + rolled(slab, 1, 1) + rolled(slab, -1, 1)
        return slab, summed + rolled(slab, 2, 2) + rolled(slab, -2, 2)

    def sweep1(field, out, radius):
        for a, b, count in near1(radius):
            slab, summed = sum1(field, a, b, count)
            fresh = KEEP * slab + read1(g1, a, b, count) * (read1(s1, a, b, count) + 0.5 * summed)
            write1(out, a, b, fresh)

    def packed(out, slabs):
        parts = [slab[z] for slab in slabs for z in range(part_z)]
        lane = lax.broadcasted_iota(jnp.int32, parts[0].shape, 1)
        values = parts[0]
        for k in range(1, len(parts)):
            values = jnp.where(lane % 4 == k, parts[k], values)
        out[ta, gz] = values

    def unpacked(source, t):
        pair, odd = divmod(t, part_t)
        values = source[pair]
        lane = lax.broadcasted_iota(jnp.int32, values.shape, 2)
        pieces = []
        for z in range(part_z):
            piece = jnp.where(lane % 4 == odd * part_z + z, values, 0.0)
            piece = piece + pair_swap(piece, 1, 2)
            pieces.append(piece + pair_swap(piece, 2, 2))
        return jnp.stack(pieces, axis=1).reshape(all_z, ngy * rows2, lanes)

    inside = list(range(1, size_t - 1))
    ends = [0, size_t - 1]

    for t in range(size_t):
        for load in loads[t]:
            load.wait()
        weight = DAMPING / (8.0 + m_ref[t])
        g0[t] = weight
        put(v0a, ys0.at[0], t, weight * s_ref[t])
    pl.semaphore_wait(barrier, len(met))
    over_t, sides = exchange0(0, v0a, ys0.at[0], y0.at[0])
    for t in range(size_t1):
        mean = halved(z_pairs(m_ref[2 * t] + m_ref[2 * t + 1]), t, 1)
        m1[t + 2, pl.ds(2, size_z1), gy] = mean
    mass_copies = spread1(0, m1)

    def sweep0(field, halos, out, faces, ts, also=None):
        for t in ts:
            slab, summed = sum0(field, halos, t)
            fresh = KEEP * slab + g0[t] * (s_ref[t] + summed)
            put(out, faces, t, fresh)
            if also is not None:
                also[t] = fresh

    finish(sides)
    sweep0(v0a, y0.at[0], v0b, ys0.at[1], inside)
    finish(over_t)
    sweep0(v0a, y0.at[0], v0b, ys0.at[1], ends)
    over_t, sides = exchange0(1, v0b, ys0.at[1], y0.at[1])
    finish(mass_copies)
    for a, b, count in near1(2):
        write1(g1, a, b, DAMPING / (4.0 + read1(m1, a, b, count)))

    def to_level2(slabs):
        return [
            halved(z_pairs(slabs[2 * t] + slabs[2 * t + 1]), t, 2) for t in range(part_t)
        ]

    packed(mall, to_level2([read1(m1, 2 + t, 2, size_z1) for t in range(size_t1)]))
    mass_copies = gather(0, mall)

    def remainder0(ts):
        for t in ts:
            remainder = []
            for odd in range(2):
                slab, summed = sum0(v0b, y0.at[1], 2 * t + odd)
                remainder.append(s_ref[2 * t + odd] + summed - (8.0 + m_ref[2 * t + odd]) * slab)
            s1[t + 2, pl.ds(2, size_z1), gy] = halved(z_pairs(remainder[0] + remainder[1]), t, 1)

    finish(sides)
    remainder0(range(1, size_t1 - 1))
    finish(over_t)
    remainder0((0, size_t1 - 1))
    source_copies = spread1(1, s1)
    finish(mass_copies)
    for t in range(all_t):
        mass = unpacked(mall, t)
        m2[t] = mass
        g2[t] = DAMPING / (2.0 + mass)
    weights3 = [
        DAMPING / (1.0 + coarse_full(m2[2 * t], m2[2 * t + 1])) for t in range(all_t // 2)
    ]
    finish(source_copies)

    for a, b, count in near1(2):
        write1(v1a, a, b, read1(g1, a, b, count) * read1(s1, a, b, count))
    sweep1(v1a, v1b, 1)
    remainder = []
    for a, b, count in near1(0):
        slab, summed = sum1(v1b, a, b, count)
        remainder.append(
            read1(s1, a, b, count) + 0.5 * summed - (4.0 + read1(m1, a, b, count)) * slab
        )
    packed(rall, to_level2(remainder))
    finish(gather(1, rall))

    for t in range(all_t):
        source = unpacked(rall, t)
        s2[t] = source
        u2[t] = g2[t] * source

    def sum2(field, t):
        slab = field[t]
        summed = field[(t - 1) % all_t] + field[(t + 1) % all_t]
        summed = summed + shifted_z(slab, True) + shifted_z(slab, False)
        summed = summed + rolled(slab, 1, 1) + rolled(slab, -1, 1)
        return slab, summed + rolled(slab, 4, 2) + rolled(slab, -4, 2)

    def sweep2(field, out):
        for t in range(all_t):
            slab, summed = sum2(field, t)
            out[t] = KEEP * slab + g2[t] * (s2[t] + 0.25 * summed)

    sweep2(u2, w2)
    sources3 = []
    for t in range(all_t // 2):
        remainder = []
        for odd in range(2):
            slab, summed = sum2(w2, 2 * t + odd)
            remainder.append(s2[2 * t + odd] + 0.25 * summed - (2.0 + m2[2 * t + odd]) * slab)
        sources3.append(coarse_full(*remainder))

    values = [weight * source for weight, source in zip(weights3, sources3)]
    count = len(values)
    for sweep_no in range(3):
        fresh = []
        for t in range(count):
            slab = values[t]
            summed = values[(t - 1) % count] + values[(t + 1) % count]
            summed = summed + shifted_z(slab, True) + shifted_z(slab, False)
            summed = summed + rolled(slab, 2, 1) + rolled(slab, -2, 1)
            summed = summed + rolled(slab, 8, 2) + rolled(slab, -8, 2)
            fresh.append(KEEP * slab + weights3[t] * (sources3[t] + 0.125 * summed))
        values = fresh

    for t in range(all_t):
        w2[t] = w2[t] + refined_z(values[t // 2])
    sweep2(w2, u2)
    sweep2(u2, w2)

    for a in range(part_t + 2):
        at_t = lax.rem(ta * part_t + (a - 1 + all_t), all_t)
        slabs = []
        for b in range(part_z + 2):
            at_z = lax.rem(gz * part_z + (b - 1 + all_z), all_z)
            slabs.append(w2[at_t, pl.ds(at_z, 1)])
        e2[a] = doubled(jnp.concatenate(slabs, axis=0), a)
    for a, b, count in near1(1):
        fine = refined_z(e2[a // 2])
        write1(v1w, a, b, read1(v1b, a, b, count) + fine[b:b + count])
    sweep1(v1w, v1x, 0)
    finish(send(
        around(v1x, (), (0,)), lambda place: fxs.at[place], lambda place: fxr.at[place],
    ))
    sweep1(v1x, e1, 1)

    under = lax.rem(gy + ngy - 1, ngy)
    over = lax.rem(gy + 1, ngy)
    for p in range(size_t + 2):
        at_t = (p + 1) // 2 + 1
        if p in (0, size_t + 1):
            fine = refined_z(doubled(e1[at_t, pl.ds(2, size_z1), gy], 0))
            v0w[p, pl.ds(1, size_z)] = v0b[p, pl.ds(1, size_z)] + fine
        else:
            if p % 2:
                fine = refined_z(doubled(e1[at_t, pl.ds(1, size_z1 + 2), gy], p // 2 % 4))
                fine = fine[1:1 + size_z + 2]
                low = refined_z(e1[at_t, pl.ds(2, size_z1), under, pl.ds(rows1 - 1, 1)])
                high = refined_z(e1[at_t, pl.ds(2, size_z1), over, pl.ds(0, 1)])
            v0w[p] = v0b[p] + fine
            y0[2, 0, p - 1] = y0[1, 0, p - 1] + low
            y0[2, 1, p - 1] = y0[1, 1, p - 1] + high
    sweep0(v0w, y0.at[2], v0x, ys0.at[2], ends + inside)
    over_t, sides = exchange0(2, v0x, ys0.at[2], y0.at[3])
    finish(sides)
    sweep0(v0x, y0.at[3], v0s, ys0.at[3], inside, sol_ref)
    finish(over_t)
    sweep0(v0x, y0.at[3], v0s, ys0.at[3], ends, sol_ref)
    over_t, sides = exchange0(3, v0s, ys0.at[3], y0.at[4])

    def residual(ts):
        for t in ts:
            slab, summed = sum0(v0s, y0.at[4], t)
            res_ref[t] = s_ref[t] + summed - (8.0 + m_ref[t]) * slab

    finish(sides)
    residual(inside)
    finish(over_t)
    residual(ends)


def coarse_full(even, odd):
    summed = even + odd
    count, rows, lanes = summed.shape
    summed = summed.reshape(count // 2, 2, rows, lanes)
    summed = summed[:, 0] + summed[:, 1]
    summed = summed + pair_swap(summed, 1, 1)
    return (summed + pair_swap(summed, 4, 2)) * 0.0625


def per_device(sizes, right_side, mass_field):
    nta, ngz, ngy = sizes
    size_t, size_z, rows, lanes = right_side.shape
    size_t1, size_z1, rows1 = size_t // 2, size_z // 2, rows // 2
    part_t, part_z, rows2 = size_t // 4, size_z // 4, rows // 4
    vmem = lambda *shape: pltpu.VMEM(shape, jnp.float32)
    dma = lambda *shape: pltpu.SemaphoreType.DMA(shape)
    padded0 = vmem(size_t + 2, size_z + 2, rows, lanes)
    padded1 = vmem(size_t1 + 4, size_z1 + 4, ngy, rows1, lanes)
    whole2 = vmem(part_t * nta, part_z * ngz, rows2 * ngy, lanes)
    packs = vmem(nta, ngz, rows2 * ngy, lanes)
    spreads, peers = 8 * ngy + ngy - 1, nta * ngz - 1
    scratch = [
        vmem(size_t, size_z, rows, lanes), padded0, padded0, padded0, padded0, padded0,
        vmem(5, 2, size_t, size_z, 1, lanes), vmem(4, 2, size_t, size_z, 1, lanes),
        vmem(max(size_t1, part_t + 2), size_z, max(rows, ngy * rows1), lanes),
        *[padded1] * 8, vmem(part_t + 2, part_z + 2, ngy * rows1, lanes),
        packs, packs, *[whole2] * 5,
        dma(4, 6), dma(4, 6), dma(2, spreads), dma(2, spreads), dma(8), dma(8),
        dma(2, peers), dma(2, peers),
        vmem(size_t, size_z, rows, lanes), vmem(size_t, size_z, rows, lanes), dma(2, size_t),
    ]
    block = jax.ShapeDtypeStruct(right_side.shape, jnp.float32)
    return pl.pallas_call(
        functools.partial(kernel, sizes),
        out_shape=(block, block),
        in_specs=[pl.BlockSpec(memory_space=pltpu.HBM)] * 2,
        out_specs=(pl.BlockSpec(memory_space=pltpu.VMEM),) * 2,
        scratch_shapes=scratch,
        compiler_params=pltpu.CompilerParams(
            collective_id=0, has_side_effects=True, vmem_limit_bytes=48 * 1024 * 1024
        ),
    )(right_side, mass_field)


def solution(mesh):
    sizes = tuple(mesh.shape[axis] for axis in ("ta", "gz", "gy"))
    spec = P("ta", "gz", "gy", None)
    return jax.shard_map(
        functools.partial(per_device, sizes),
        mesh=mesh,
        in_specs=(spec, spec),
        out_specs=(spec, spec),
        check_vma=False,
    )
```

```python
import functools

import jax
import jax.numpy as jnp
from jax import lax
from jax.experimental import pallas as pl
from jax.experimental.pallas import tpu as pltpu
from jax.sharding import PartitionSpec as P

DAMPING = 0.7
KEEP = 1.0 - DAMPING
MESH = pl.DeviceIdType.MESH


def rolled(values, shift, axis):
    return pltpu.roll(values, shift % values.shape[axis], axis)


def pair_swap(values, step, axis):
    index = lax.broadcasted_iota(jnp.int32, values.shape, axis)
    return jnp.where((index // step) % 2 == 0, rolled(values, -step, axis), rolled(values, step, axis))


def z_pairs(summed):
    count, rows, lanes = summed.shape
    summed = summed.reshape(count // 2, 2, rows, lanes)
    return summed[:, 0] + summed[:, 1]


def refined_z(slab):
    return jnp.repeat(slab, 2, axis=0)


def shifted_z(slab, forward):
    if forward:
        return jnp.concatenate([slab[-1:], slab[:-1]], axis=0)
    return jnp.concatenate([slab[1:], slab[:1]], axis=0)


def kernel(sizes, s_hbm, m_hbm, sol_ref, res_ref, *scratch):
    nta, ngz, ngy = sizes
    (g0, v0a, v0b, v0w, v0x, v0s, y0, ys0, fold,
     s1, m1, g1, v1a, v1b, v1w, v1x, e1, e2,
     mall, rall, s2, m2, g2, u2, w2,
     f0s, f0r, f1s, f1r, fxs, fxr, gsend, grecv, s_ref, m_ref, loaded) = scratch
    size_t, size_z, rows, lanes = s_ref.shape
    size_t1, size_z1, rows1 = size_t // 2, size_z // 2, rows // 2
    part_t, part_z, rows2 = size_t // 4, size_z // 4, rows // 4
    all_t, all_z = part_t * nta, part_z * ngz
    ta, gz, gy = lax.axis_index("ta"), lax.axis_index("gz"), lax.axis_index("gy")

    first_up = lax.min(ta, 1)

    def device(dt, dz, dy):
        return {
            "ta": lax.rem(ta + dt + nta, nta),
            "gz": lax.rem(gz + dz + ngz, ngz),
            "gy": lax.rem(gy + dy + ngy, ngy),
        }

    near = [(dt, dz, dy) for dt in (-1, 0, 1) for dz in (-1, 0, 1) for dy in range(ngy)]
    across = [(dt, dz, 0) for dt in reversed(range(nta)) for dz in range(ngz) if dt or dz]
    loads = []
    for t in range(size_t):
        loads.append((
            pltpu.make_async_copy(m_hbm.at[pl.ds(t, 1)], m_ref.at[pl.ds(t, 1)], loaded.at[0, t]),
            pltpu.make_async_copy(s_hbm.at[pl.ds(t, 1)], s_ref.at[pl.ds(t, 1)], loaded.at[1, t]),
        ))
    met = sorted({(dt % nta, dz % ngz, dy % ngy) for dt, dz, dy in near + across} - {(0, 0, 0)})
    barrier = pltpu.get_barrier_semaphore()
    for offset in met:
        pl.semaphore_signal(barrier, inc=1, device_id=device(*offset), device_id_type=MESH)
    for t in [0, size_t - 1] + list(range(1, size_t - 1)):
        for load in loads[t]:
            load.start()

    def send(moves, sends, receives):
        copies = [
            pltpu.make_async_remote_copy(
                src_ref=source, dst_ref=target, send_sem=sends(place), recv_sem=receives(place),
                device_id=device(*offset), device_id_type=MESH,
            )
            for place, source, target, offset in moves
        ]
        for copy in copies:
            copy.start()
        sent.extend(copies)
        return copies

    def finish(copies):
        for copy in copies:
            copy.wait_recv()

    sent = []

    def finish_sends(copies):
        for copy in copies:
            copy.wait_send()

    inner_t, inner_z = pl.ds(1, size_t), pl.ds(1, size_z)

    def send0(number, moves):
        return send(moves, lambda place: f0s.at[number, place], lambda place: f0r.at[number, place])

    def exchange_t(number, field):
        moves = []
        for up in (first_up, 1 - first_up):
            here, there = pl.ds(1 + (size_t - 1) * up, 1), pl.ds((size_t + 1) * (1 - up), 1)
            moves.append((up, field.at[here, inner_z], field.at[there, inner_z], (2 * up - 1, 0, 0)))
        return send0(number, moves)

    def exchange_sides(number, field, faces, halos):
        return send0(number, [
            (2, field.at[inner_t, pl.ds(size_z, 1)], field.at[inner_t, pl.ds(0, 1)], (0, 1, 0)),
            (3, field.at[inner_t, pl.ds(1, 1)], field.at[inner_t, pl.ds(size_z + 1, 1)], (0, -1, 0)),
            (4, faces.at[1], halos.at[0], (0, 0, 1)),
            (5, faces.at[0], halos.at[1], (0, 0, -1)),
        ])

    def around(field, part, dys):
        own_t, own_z = pl.ds(2, size_t1), pl.ds(2, size_z1)

        def span(size, deep, up):
            return pl.ds(2 + (size - deep) * up, deep), pl.ds(2 + size - (size + deep) * up, deep)

        moves = []
        for up in (first_up, 1 - first_up):
            here, there = span(size_t1, 2, up)
            for dy in dys:
                moves.append((
                    8 * dy + up, field.at[(here, own_z) + part], field.at[(there, own_z) + part],
                    (2 * up - 1, 0, dy),
                ))
        for up in (1, 0):
            here_t, there_t = span(size_t1, 1, up)
            for up_z in (1, 0):
                here_z, there_z = span(size_z1, 1, up_z)
                for dy in dys:
                    moves.append((
                        8 * dy + 2 + 2 * up + up_z,
                        field.at[(here_t, here_z) + part], field.at[(there_t, there_z) + part],
                        (2 * up - 1, 2 * up_z - 1, dy),
                    ))
        for up in (1, 0):
            here, there = span(size_z1, 2, up)
            for dy in dys:
                moves.append((
                    8 * dy + 6 + up, field.at[(own_t, here) + part], field.at[(own_t, there) + part],
                    (0, 2 * up - 1, dy),
                ))
        return moves

    def spread1(number, field):
        own = field.at[pl.ds(2, size_t1), pl.ds(2, size_z1), pl.ds(gy, 1)]
        moves = around(field, (pl.ds(gy, 1),), range(ngy))
        moves += [(8 * ngy + dy - 1, own, own, (0, 0, dy)) for dy in range(1, ngy)]
        return send(moves, lambda place: f1s.at[number, place], lambda place: f1r.at[number, place])

    def gather(number, field):
        own = field.at[ta, gz]
        return send(
            [(place, own, own, offset) for place, offset in enumerate(across)],
            lambda place: gsend.at[number, place], lambda place: grecv.at[number, place],
        )

    def put(field, faces, t, slab):
        field[t + 1, pl.ds(1, size_z)] = slab
        faces[0, t] = slab[:, :1]
        faces[1, t] = slab[:, rows - 1:]

    def sum0(field, halos, t):
        slab = field[t + 1, pl.ds(1, size_z)]
        row = lax.broadcasted_iota(jnp.int32, slab.shape, 1)
        summed = field[t, pl.ds(1, size_z)] + field[t + 2, pl.ds(1, size_z)]
        summed = summed + field[t + 1, pl.ds(0, size_z)] + field[t + 1, pl.ds(2, size_z)]
        summed = summed + jnp.where(row == 0, halos[0, t], rolled(slab, 1, 1))
        summed = summed + jnp.where(row == rows - 1, halos[1, t], rolled(slab, -1, 1))
        return slab, summed + rolled(slab, 1, 2) + rolled(slab, -1, 2)

    def halved(summed, place, step):
        count, high, _ = summed.shape
        view = fold.at[place, pl.ds(0, count)]
        view[...] = summed
        summed = view[:, pl.ds(0, high // 2, stride=2), :] + view[:, pl.ds(1, high // 2, stride=2), :]
        return (summed + pair_swap(summed, step, 2)) * 0.0625

    def doubled(slab, place):
        count, high, _ = slab.shape
        view = fold.at[place, pl.ds(0, count)]
        view[:, pl.ds(0, high, stride=2), :] = slab
        view[:, pl.ds(1, high, stride=2), :] = slab
        return view[...]

    full = ngy * rows1

    def near1(radius):
        for a in range(2 - radius, 2 + size_t1 + radius):
            reach = radius - max(2 - a, a - 1 - size_t1, 0)
            yield a, 2 - reach, size_z1 + 2 * reach

    def read1(field, a, b, count):
        return field[a, pl.ds(b, count)].reshape(count, full, lanes)

    def write1(field, a, b, slab):
        field[a, pl.ds(b, slab.shape[0])] = slab.reshape(slab.shape[0], ngy, rows1, lanes)

    def sum1(field, a, b, count):
        slab = read1(field, a, b, count)
        summed = read1(field, a - 1, b, count) + read1(field, a + 1, b, count)
        summed = summed + read1(field, a, b - 1, count) + read1(field, a, b + 1, count)
        summed = summed + rolled(slab, 1, 1) + rolled(slab, -1, 1)
        return slab, summed + rolled(slab, 2, 2) + rolled(slab, -2, 2)

    def sweep1(field, out, radius):
        for a, b, count in near1(radius):
            slab, summed = sum1(field, a, b, count)
            fresh = KEEP * slab + read1(g1, a, b, count) * (read1(s1, a, b, count) + 0.5 * summed)
            write1(out, a, b, fresh)

    def packed(out, slabs):
        parts = [slab[z] for slab in slabs for z in range(part_z)]
        lane = lax.broadcasted_iota(jnp.int32, parts[0].shape, 1)
        values = parts[0]
        for k in range(1, len(parts)):
            values = jnp.where(lane % 4 == k, parts[k], values)
        out[ta, gz] = values

    def unpacked(source, t):
        pair, odd = divmod(t, part_t)
        values = source[pair]
        lane = lax.broadcasted_iota(jnp.int32, values.shape, 2)
        pieces = []
        for z in range(part_z):
            piece = jnp.where(lane % 4 == odd * part_z + z, values, 0.0)
            piece = piece + pair_swap(piece, 1, 2)
            pieces.append(piece + pair_swap(piece, 2, 2))
        return jnp.stack(pieces, axis=1).reshape(all_z, ngy * rows2, lanes)

    inside = list(range(1, size_t - 1))
    ends = [0, size_t - 1]

    def first0(ts):
        for t in ts:
            for load in loads[t]:
                load.wait()
            weight = DAMPING / (8.0 + m_ref[t])
            g0[t] = weight
            put(v0a, ys0.at[0], t, weight * s_ref[t])

    first0(ends + inside)
    pl.semaphore_wait(barrier, len(met))
    over_t = exchange_t(0, v0a)
    sides = exchange_sides(0, v0a, ys0.at[0], y0.at[0])
    for t in range(size_t1):
        mean = halved(z_pairs(m_ref[2 * t] + m_ref[2 * t + 1]), t, 1)
        m1[t + 2, pl.ds(2, size_z1), gy] = mean
    mass_copies = spread1(0, m1)

    def sweep0(field, halos, out, faces, ts, also=None):
        for t in ts:
            slab, summed = sum0(field, halos, t)
            fresh = KEEP * slab + g0[t] * (s_ref[t] + summed)
            put(out, faces, t, fresh)
            if also is not None:
                also[t] = fresh

    finish(sides)
    sweep0(v0a, y0.at[0], v0b, ys0.at[1], inside)
    finish(over_t)
    sweep0(v0a, y0.at[0], v0b, ys0.at[1], ends)
    over_t = exchange_t(1, v0b)
    sides = exchange_sides(1, v0b, ys0.at[1], y0.at[1])
    finish(mass_copies)
    for a, b, count in near1(2):
        write1(g1, a, b, DAMPING / (4.0 + read1(m1, a, b, count)))

    def to_level2(slabs):
        return [
            halved(z_pairs(slabs[2 * t] + slabs[2 * t + 1]), t, 2) for t in range(part_t)
        ]

    packed(mall, to_level2([read1(m1, 2 + t, 2, size_z1) for t in range(size_t1)]))
    mass_copies = gather(0, mall)

    def remainder0(ts):
        for t in ts:
            remainder = []
            for odd in range(2):
                slab, summed = sum0(v0b, y0.at[1], 2 * t + odd)
                remainder.append(s_ref[2 * t + odd] + summed - (8.0 + m_ref[2 * t + odd]) * slab)
            s1[t + 2, pl.ds(2, size_z1), gy] = halved(z_pairs(remainder[0] + remainder[1]), t, 1)

    finish(sides)
    remainder0(range(1, size_t1 - 1))
    finish(over_t)
    remainder0((0, size_t1 - 1))
    source_copies = spread1(1, s1)
    finish(mass_copies)
    for t in range(all_t):
        mass = unpacked(mall, t)
        m2[t] = mass
        g2[t] = DAMPING / (2.0 + mass)
    weights3 = [
        DAMPING / (1.0 + coarse_full(m2[2 * t], m2[2 * t + 1])) for t in range(all_t // 2)
    ]
    finish(source_copies)

    for a, b, count in near1(2):
        write1(v1a, a, b, read1(g1, a, b, count) * read1(s1, a, b, count))
    sweep1(v1a, v1b, 1)
    remainder = []
    for a, b, count in near1(0):
        slab, summed = sum1(v1b, a, b, count)
        remainder.append(
            read1(s1, a, b, count) + 0.5 * summed - (4.0 + read1(m1, a, b, count)) * slab
        )
    packed(rall, to_level2(remainder))
    finish(gather(1, rall))

    for t in range(all_t):
        source = unpacked(rall, t)
        s2[t] = source
        u2[t] = g2[t] * source

    def sum2(field, t):
        slab = field[t]
        summed = field[(t - 1) % all_t] + field[(t + 1) % all_t]
        summed = summed + shifted_z(slab, True) + shifted_z(slab, False)
        summed = summed + rolled(slab, 1, 1) + rolled(slab, -1, 1)
        return slab, summed + rolled(slab, 4, 2) + rolled(slab, -4, 2)

    def sweep2(field, out):
        for t in range(all_t):
            slab, summed = sum2(field, t)
            out[t] = KEEP * slab + g2[t] * (s2[t] + 0.25 * summed)

    sweep2(u2, w2)
    sources3 = []
    for t in range(all_t // 2):
        remainder = []
        for odd in range(2):
            slab, summed = sum2(w2, 2 * t + odd)
            remainder.append(s2[2 * t + odd] + 0.25 * summed - (2.0 + m2[2 * t + odd]) * slab)
        sources3.append(coarse_full(*remainder))

    values = [weight * source for weight, source in zip(weights3, sources3)]
    count = len(values)
    for sweep_no in range(3):
        fresh = []
        for t in range(count):
            slab = values[t]
            summed = values[(t - 1) % count] + values[(t + 1) % count]
            summed = summed + shifted_z(slab, True) + shifted_z(slab, False)
            summed = summed + rolled(slab, 2, 1) + rolled(slab, -2, 1)
            summed = summed + rolled(slab, 8, 2) + rolled(slab, -8, 2)
            fresh.append(KEEP * slab + weights3[t] * (sources3[t] + 0.125 * summed))
        values = fresh

    for t in range(all_t):
        w2[t] = w2[t] + refined_z(values[t // 2])
    sweep2(w2, u2)
    sweep2(u2, w2)

    for a in range(part_t + 2):
        at_t = lax.rem(ta * part_t + (a - 1 + all_t), all_t)
        slabs = []
        for b in range(part_z + 2):
            at_z = lax.rem(gz * part_z + (b - 1 + all_z), all_z)
            slabs.append(w2[at_t, pl.ds(at_z, 1)])
        e2[a] = doubled(jnp.concatenate(slabs, axis=0), a)
    for a, b, count in near1(1):
        fine = refined_z(e2[a // 2])
        write1(v1w, a, b, read1(v1b, a, b, count) + fine[b:b + count])
    sweep1(v1w, v1x, 0)
    finish(send(
        around(v1x, (), (0,)), lambda place: fxs.at[place], lambda place: fxr.at[place],
    ))
    sweep1(v1x, e1, 1)

    under = lax.rem(gy + ngy - 1, ngy)
    over = lax.rem(gy + 1, ngy)
    def corrected0(layers):
        for at_t in layers:
            own = [p for p in (2 * at_t - 3, 2 * at_t - 2) if 1 <= p <= size_t]
            if not own:
                p = 0 if at_t == 1 else size_t + 1
                fine = refined_z(doubled(e1[at_t, pl.ds(2, size_z1), gy], 0))
                v0w[p, inner_z] = v0b[p, inner_z] + fine
                continue
            fine = refined_z(doubled(e1[at_t, pl.ds(1, size_z1 + 2), gy], at_t % 4))
            fine = fine[1:1 + size_z + 2]
            low = refined_z(e1[at_t, pl.ds(2, size_z1), under, pl.ds(rows1 - 1, 1)])
            high = refined_z(e1[at_t, pl.ds(2, size_z1), over, pl.ds(0, 1)])
            for p in own:
                v0w[p] = v0b[p] + fine
                y0[2, 0, p - 1] = y0[1, 0, p - 1] + low
                y0[2, 1, p - 1] = y0[1, 1, p - 1] + high

    corrected0((1, 2, size_t1 + 1, size_t1 + 2))
    sweep0(v0w, y0.at[2], v0x, ys0.at[2], ends)
    over_t = exchange_t(2, v0x)
    corrected0(range(3, size_t1 + 1))
    sweep0(v0w, y0.at[2], v0x, ys0.at[2], inside)
    sides = exchange_sides(2, v0x, ys0.at[2], y0.at[3])
    finish(sides)
    sweep0(v0x, y0.at[3], v0s, ys0.at[3], inside, sol_ref)
    finish(over_t)
    sweep0(v0x, y0.at[3], v0s, ys0.at[3], ends, sol_ref)
    earlier = len(sent)
    over_t = exchange_t(3, v0s)
    sides = exchange_sides(3, v0s, ys0.at[3], y0.at[4])
    finish_sends(sent[:earlier])

    def residual(ts):
        for t in ts:
            slab, summed = sum0(v0s, y0.at[4], t)
            res_ref[t] = s_ref[t] + summed - (8.0 + m_ref[t]) * slab

    finish(sides)
    residual(inside)
    finish(over_t)
    residual(ends)
    finish_sends(sent[earlier:])


def coarse_full(even, odd):
    summed = even + odd
    count, rows, lanes = summed.shape
    summed = summed.reshape(count // 2, 2, rows, lanes)
    summed = summed[:, 0] + summed[:, 1]
    summed = summed + pair_swap(summed, 1, 1)
    return (summed + pair_swap(summed, 4, 2)) * 0.0625


def per_device(sizes, right_side, mass_field):
    nta, ngz, ngy = sizes
    size_t, size_z, rows, lanes = right_side.shape
    size_t1, size_z1, rows1 = size_t // 2, size_z // 2, rows // 2
    part_t, part_z, rows2 = size_t // 4, size_z // 4, rows // 4
    vmem = lambda *shape: pltpu.VMEM(shape, jnp.float32)
    dma = lambda *shape: pltpu.SemaphoreType.DMA(shape)
    padded0 = vmem(size_t + 2, size_z + 2, rows, lanes)
    padded1 = vmem(size_t1 + 4, size_z1 + 4, ngy, rows1, lanes)
    whole2 = vmem(part_t * nta, part_z * ngz, rows2 * ngy, lanes)
    packs = vmem(nta, ngz, rows2 * ngy, lanes)
    spreads, peers = 8 * ngy + ngy - 1, nta * ngz - 1
    scratch = [
        vmem(size_t, size_z, rows, lanes), padded0, padded0, padded0, padded0, padded0,
        vmem(5, 2, size_t, size_z, 1, lanes), vmem(4, 2, size_t, size_z, 1, lanes),
        vmem(max(size_t1, part_t + 2), size_z, max(rows, ngy * rows1), lanes),
        *[padded1] * 8, vmem(part_t + 2, part_z + 2, ngy * rows1, lanes),
        packs, packs, *[whole2] * 5,
        dma(4, 6), dma(4, 6), dma(2, spreads), dma(2, spreads), dma(8), dma(8),
        dma(2, peers), dma(2, peers),
        vmem(size_t, size_z, rows, lanes), vmem(size_t, size_z, rows, lanes), dma(2, size_t),
    ]
    block = jax.ShapeDtypeStruct(right_side.shape, jnp.float32)
    return pl.pallas_call(
        functools.partial(kernel, sizes),
        out_shape=(block, block),
        in_specs=[pl.BlockSpec(memory_space=pltpu.HBM)] * 2,
        out_specs=(pl.BlockSpec(memory_space=pltpu.VMEM),) * 2,
        scratch_shapes=scratch,
        compiler_params=pltpu.CompilerParams(
            collective_id=0, has_side_effects=True, vmem_limit_bytes=48 * 1024 * 1024
        ),
    )(right_side, mass_field)


def solution(mesh):
    sizes = tuple(mesh.shape[axis] for axis in ("ta", "gz", "gy"))
    spec = P("ta", "gz", "gy", None)
    return jax.shard_map(
        functools.partial(per_device, sizes),
        mesh=mesh,
        in_specs=(spec, spec),
        out_specs=(spec, spec),
        check_vma=False,
    )
```

```python
import functools

import jax
import jax.numpy as jnp
from jax import lax
from jax.experimental import pallas as pl
from jax.experimental.pallas import tpu as pltpu
from jax.sharding import PartitionSpec as P

DAMPING = 0.7
KEEP = 1.0 - DAMPING
MESH = pl.DeviceIdType.MESH


def rolled(values, shift, axis):
    return pltpu.roll(values, shift % values.shape[axis], axis)


def pair_swap(values, step, axis):
    index = lax.broadcasted_iota(jnp.int32, values.shape, axis)
    return jnp.where((index // step) % 2 == 0, rolled(values, -step, axis), rolled(values, step, axis))


def z_pairs(summed):
    count, rows, lanes = summed.shape
    summed = summed.reshape(count // 2, 2, rows, lanes)
    return summed[:, 0] + summed[:, 1]


def refined_z(slab):
    return jnp.repeat(slab, 2, axis=0)


def shifted_z(slab, forward):
    if forward:
        return jnp.concatenate([slab[-1:], slab[:-1]], axis=0)
    return jnp.concatenate([slab[1:], slab[:1]], axis=0)


def kernel(sizes, s_hbm, m_hbm, sol_ref, res_ref, *scratch):
    nta, ngz, ngy = sizes
    (g0, v0a, v0b, v0w, v0x, v0s, y0, ys0, fold,
     s1, m1, g1, v1a, v1b, v1w, v1x, e1, e2,
     mall, rall, s2, m2, g2, u2, w2,
     f0s, f0r, f1s, f1r, fxs, fxr, gsend, grecv, s_ref, m_ref, loaded) = scratch
    size_t, size_z, rows, lanes = s_ref.shape
    size_t1, size_z1, rows1 = size_t // 2, size_z // 2, rows // 2
    part_t, part_z, rows2 = size_t // 4, size_z // 4, rows // 4
    all_t, all_z = part_t * nta, part_z * ngz
    ta, gz, gy = lax.axis_index("ta"), lax.axis_index("gz"), lax.axis_index("gy")

    first_up = lax.min(ta, 1)

    def device(dt, dz, dy):
        return {
            "ta": lax.rem(ta + dt + nta, nta),
            "gz": lax.rem(gz + dz + ngz, ngz),
            "gy": lax.rem(gy + dy + ngy, ngy),
        }

    near = [(dt, dz, dy) for dt in (-1, 0, 1) for dz in (-1, 0, 1) for dy in range(ngy)]
    across = [(dt, dz, 0) for dt in reversed(range(nta)) for dz in range(ngz) if dt or dz]
    loads = []
    for t in range(size_t):
        loads.append((
            pltpu.make_async_copy(m_hbm.at[pl.ds(t, 1)], m_ref.at[pl.ds(t, 1)], loaded.at[0, t]),
            pltpu.make_async_copy(s_hbm.at[pl.ds(t, 1)], s_ref.at[pl.ds(t, 1)], loaded.at[1, t]),
        ))
    met = sorted({(dt % nta, dz % ngz, dy % ngy) for dt, dz, dy in near + across} - {(0, 0, 0)})
    barrier = pltpu.get_barrier_semaphore()
    for offset in met:
        pl.semaphore_signal(barrier, inc=1, device_id=device(*offset), device_id_type=MESH)
    for t in [0, size_t - 1] + list(range(1, size_t - 1)):
        for load in loads[t]:
            load.start()

    def send(moves, sends, receives):
        copies = [
            pltpu.make_async_remote_copy(
                src_ref=source, dst_ref=target, send_sem=sends(place), recv_sem=receives(place),
                device_id=device(*offset), device_id_type=MESH,
            )
            for place, source, target, offset in moves
        ]
        for copy in copies:
            copy.start()
        sent.extend(copies)
        return copies

    def finish(copies):
        for copy in copies:
            copy.wait_recv()

    sent = []

    def finish_sends(copies):
        for copy in copies:
            copy.wait_send()

    inner_t, inner_z = pl.ds(1, size_t), pl.ds(1, size_z)

    def send0(number, moves):
        return send(moves, lambda place: f0s.at[number, place], lambda place: f0r.at[number, place])

    def exchange_t(number, field):
        moves = []
        for up in (first_up, 1 - first_up):
            here, there = pl.ds(1 + (size_t - 1) * up, 1), pl.ds((size_t + 1) * (1 - up), 1)
            moves.append((up, field.at[here, inner_z], field.at[there, inner_z], (2 * up - 1, 0, 0)))
        return send0(number, moves)

    def exchange_sides(number, field, faces, halos):
        return send0(number, [
            (2, field.at[inner_t, pl.ds(size_z, 1)], field.at[inner_t, pl.ds(0, 1)], (0, 1, 0)),
            (3, field.at[inner_t, pl.ds(1, 1)], field.at[inner_t, pl.ds(size_z + 1, 1)], (0, -1, 0)),
            (4, faces.at[1], halos.at[0], (0, 0, 1)),
            (5, faces.at[0], halos.at[1], (0, 0, -1)),
        ])

    def around(field, part, dys, deep=2):
        own_t, own_z = pl.ds(2, size_t1), pl.ds(2, size_z1)

        def span(size, deep, up):
            return pl.ds(2 + (size - deep) * up, deep), pl.ds(2 + size - (size + deep) * up, deep)

        moves = []
        for up in (first_up, 1 - first_up):
            here, there = span(size_t1, deep, up)
            for dy in dys:
                moves.append((
                    8 * dy + up, field.at[(here, own_z) + part], field.at[(there, own_z) + part],
                    (2 * up - 1, 0, dy),
                ))
        for up in (1, 0) if deep > 1 else ():
            here_t, there_t = span(size_t1, 1, up)
            for up_z in (1, 0):
                here_z, there_z = span(size_z1, 1, up_z)
                for dy in dys:
                    moves.append((
                        8 * dy + 2 + 2 * up + up_z,
                        field.at[(here_t, here_z) + part], field.at[(there_t, there_z) + part],
                        (2 * up - 1, 2 * up_z - 1, dy),
                    ))
        for up in (1, 0):
            here, there = span(size_z1, deep, up)
            for dy in dys:
                moves.append((
                    8 * dy + 6 + up, field.at[(own_t, here) + part], field.at[(own_t, there) + part],
                    (0, 2 * up - 1, dy),
                ))
        return moves

    def spread1(number, field, deep):
        own = field.at[pl.ds(2, size_t1), pl.ds(2, size_z1), pl.ds(gy, 1)]
        moves = around(field, (pl.ds(gy, 1),), range(ngy), deep)
        moves += [(8 * ngy + dy - 1, own, own, (0, 0, dy)) for dy in range(1, ngy)]
        return send(moves, lambda place: f1s.at[number, place], lambda place: f1r.at[number, place])

    def gather(number, field):
        own = field.at[ta, gz]
        return send(
            [(place, own, own, offset) for place, offset in enumerate(across)],
            lambda place: gsend.at[number, place], lambda place: grecv.at[number, place],
        )

    def put(field, faces, t, slab):
        field[t + 1, pl.ds(1, size_z)] = slab
        faces[0, t] = slab[:, :1]
        faces[1, t] = slab[:, rows - 1:]

    def sum0(field, halos, t):
        slab = field[t + 1, pl.ds(1, size_z)]
        row = lax.broadcasted_iota(jnp.int32, slab.shape, 1)
        summed = field[t, pl.ds(1, size_z)] + field[t + 2, pl.ds(1, size_z)]
        summed = summed + field[t + 1, pl.ds(0, size_z)] + field[t + 1, pl.ds(2, size_z)]
        summed = summed + jnp.where(row == 0, halos[0, t], rolled(slab, 1, 1))
        summed = summed + jnp.where(row == rows - 1, halos[1, t], rolled(slab, -1, 1))
        return slab, summed + rolled(slab, 1, 2) + rolled(slab, -1, 2)

    def halved(summed, place, step):
        count, high, _ = summed.shape
        view = fold.at[place, pl.ds(0, count)]
        view[...] = summed
        summed = view[:, pl.ds(0, high // 2, stride=2), :] + view[:, pl.ds(1, high // 2, stride=2), :]
        return (summed + pair_swap(summed, step, 2)) * 0.0625

    def doubled(slab, place):
        count, high, _ = slab.shape
        view = fold.at[place, pl.ds(0, count)]
        view[:, pl.ds(0, high, stride=2), :] = slab
        view[:, pl.ds(1, high, stride=2), :] = slab
        return view[...]

    full = ngy * rows1

    def near1(radius):
        for a in range(2 - radius, 2 + size_t1 + radius):
            reach = radius - max(2 - a, a - 1 - size_t1, 0)
            yield a, 2 - reach, size_z1 + 2 * reach

    def read1(field, a, b, count):
        return field[a, pl.ds(b, count)].reshape(count, full, lanes)

    def write1(field, a, b, slab):
        field[a, pl.ds(b, slab.shape[0])] = slab.reshape(slab.shape[0], ngy, rows1, lanes)

    def sum1(field, a, b, count):
        slab = read1(field, a, b, count)
        summed = read1(field, a - 1, b, count) + read1(field, a + 1, b, count)
        summed = summed + read1(field, a, b - 1, count) + read1(field, a, b + 1, count)
        summed = summed + rolled(slab, 1, 1) + rolled(slab, -1, 1)
        return slab, summed + rolled(slab, 2, 2) + rolled(slab, -2, 2)

    def sweep1(field, out, radius):
        for a, b, count in near1(radius):
            slab, summed = sum1(field, a, b, count)
            fresh = KEEP * slab + read1(g1, a, b, count) * (read1(s1, a, b, count) + 0.5 * summed)
            write1(out, a, b, fresh)

    def packed(out, slabs):
        parts = [slab[z] for slab in slabs for z in range(part_z)]
        lane = lax.broadcasted_iota(jnp.int32, parts[0].shape, 1)
        values = parts[0]
        for k in range(1, len(parts)):
            values = jnp.where(lane % 4 == k, parts[k], values)
        out[ta, gz] = values

    def unpacked(source, t):
        pair, odd = divmod(t, part_t)
        values = source[pair]
        lane = lax.broadcasted_iota(jnp.int32, values.shape, 2)
        pieces = []
        for z in range(part_z):
            piece = jnp.where(lane % 4 == odd * part_z + z, values, 0.0)
            piece = piece + pair_swap(piece, 1, 2)
            pieces.append(piece + pair_swap(piece, 2, 2))
        return jnp.stack(pieces, axis=1).reshape(all_z, ngy * rows2, lanes)

    inside = list(range(1, size_t - 1))
    ends = [0, size_t - 1]

    def first0(ts):
        for t in ts:
            for load in loads[t]:
                load.wait()
            weight = DAMPING / (8.0 + m_ref[t])
            g0[t] = weight
            put(v0a, ys0.at[0], t, weight * s_ref[t])

    first0(ends + inside)
    pl.semaphore_wait(barrier, len(met))
    over_t = exchange_t(0, v0a)
    sides = exchange_sides(0, v0a, ys0.at[0], y0.at[0])
    for t in range(size_t1):
        mean = halved(z_pairs(m_ref[2 * t] + m_ref[2 * t + 1]), t, 1)
        m1[t + 2, pl.ds(2, size_z1), gy] = mean
    mass_copies = spread1(0, m1, 1)

    def sweep0(field, halos, out, faces, ts, also=None):
        for t in ts:
            slab, summed = sum0(field, halos, t)
            fresh = KEEP * slab + g0[t] * (s_ref[t] + summed)
            put(out, faces, t, fresh)
            if also is not None:
                also[t] = fresh

    finish(sides)
    sweep0(v0a, y0.at[0], v0b, ys0.at[1], inside)
    finish(over_t)
    sweep0(v0a, y0.at[0], v0b, ys0.at[1], ends)
    over_t = exchange_t(1, v0b)
    sides = exchange_sides(1, v0b, ys0.at[1], y0.at[1])
    finish(mass_copies)
    for a, b, count in near1(1):
        write1(g1, a, b, DAMPING / (4.0 + read1(m1, a, b, count)))

    def to_level2(slabs):
        return [
            halved(z_pairs(slabs[2 * t] + slabs[2 * t + 1]), t, 2) for t in range(part_t)
        ]

    packed(mall, to_level2([read1(m1, 2 + t, 2, size_z1) for t in range(size_t1)]))
    mass_copies = gather(0, mall)

    def remainder0(ts):
        for t in ts:
            remainder = []
            for odd in range(2):
                slab, summed = sum0(v0b, y0.at[1], 2 * t + odd)
                remainder.append(s_ref[2 * t + odd] + summed - (8.0 + m_ref[2 * t + odd]) * slab)
            weight = g1[t + 2, pl.ds(2, size_z1), gy]
            source = halved(z_pairs(remainder[0] + remainder[1]), t, 1)
            v1a[t + 2, pl.ds(2, size_z1), gy] = weight * source

    finish(sides)
    remainder0(range(1, size_t1 - 1))
    finish(over_t)
    remainder0((0, size_t1 - 1))
    source_copies = spread1(1, v1a, 2)
    finish(mass_copies)
    for t in range(all_t):
        mass = unpacked(mall, t)
        m2[t] = mass
        g2[t] = DAMPING / (2.0 + mass)
    weights3 = [
        DAMPING / (1.0 + coarse_full(m2[2 * t], m2[2 * t + 1])) for t in range(all_t // 2)
    ]
    finish(source_copies)

    for a, b, count in near1(1):
        scale = (4.0 + read1(m1, a, b, count)) * (1.0 / DAMPING)
        write1(s1, a, b, read1(v1a, a, b, count) * scale)
    sweep1(v1a, v1b, 1)
    remainder = []
    for a, b, count in near1(0):
        slab, summed = sum1(v1b, a, b, count)
        remainder.append(
            read1(s1, a, b, count) + 0.5 * summed - (4.0 + read1(m1, a, b, count)) * slab
        )
    packed(rall, to_level2(remainder))
    finish(gather(1, rall))

    for t in range(all_t):
        source = unpacked(rall, t)
        s2[t] = source
        u2[t] = g2[t] * source

    def sum2(field, t):
        slab = field[t]
        summed = field[(t - 1) % all_t] + field[(t + 1) % all_t]
        summed = summed + shifted_z(slab, True) + shifted_z(slab, False)
        summed = summed + rolled(slab, 1, 1) + rolled(slab, -1, 1)
        return slab, summed + rolled(slab, 4, 2) + rolled(slab, -4, 2)

    def sweep2(field, out):
        for t in range(all_t):
            slab, summed = sum2(field, t)
            out[t] = KEEP * slab + g2[t] * (s2[t] + 0.25 * summed)

    sweep2(u2, w2)
    sources3 = []
    for t in range(all_t // 2):
        remainder = []
        for odd in range(2):
            slab, summed = sum2(w2, 2 * t + odd)
            remainder.append(s2[2 * t + odd] + 0.25 * summed - (2.0 + m2[2 * t + odd]) * slab)
        sources3.append(coarse_full(*remainder))

    values = [weight * source for weight, source in zip(weights3, sources3)]
    count = len(values)
    for sweep_no in range(3):
        fresh = []
        for t in range(count):
            slab = values[t]
            summed = values[(t - 1) % count] + values[(t + 1) % count]
            summed = summed + shifted_z(slab, True) + shifted_z(slab, False)
            summed = summed + rolled(slab, 2, 1) + rolled(slab, -2, 1)
            summed = summed + rolled(slab, 8, 2) + rolled(slab, -8, 2)
            fresh.append(KEEP * slab + weights3[t] * (sources3[t] + 0.125 * summed))
        values = fresh

    for t in range(all_t):
        w2[t] = w2[t] + refined_z(values[t // 2])
    sweep2(w2, u2)
    sweep2(u2, w2)

    for a in range(part_t + 2):
        at_t = lax.rem(ta * part_t + (a - 1 + all_t), all_t)
        slabs = []
        for b in range(part_z + 2):
            at_z = lax.rem(gz * part_z + (b - 1 + all_z), all_z)
            slabs.append(w2[at_t, pl.ds(at_z, 1)])
        e2[a] = doubled(jnp.concatenate(slabs, axis=0), a)
    for a, b, count in near1(1):
        fine = refined_z(e2[a // 2])
        write1(v1w, a, b, read1(v1b, a, b, count) + fine[b:b + count])
    sweep1(v1w, v1x, 0)
    finish(send(
        around(v1x, (), (0,)), lambda place: fxs.at[place], lambda place: fxr.at[place],
    ))
    sweep1(v1x, e1, 1)

    under = lax.rem(gy + ngy - 1, ngy)
    over = lax.rem(gy + 1, ngy)
    def corrected0(layers):
        for at_t in layers:
            own = [p for p in (2 * at_t - 3, 2 * at_t - 2) if 1 <= p <= size_t]
            if not own:
                p = 0 if at_t == 1 else size_t + 1
                fine = refined_z(doubled(e1[at_t, pl.ds(2, size_z1), gy], 0))
                v0w[p, inner_z] = v0b[p, inner_z] + fine
                continue
            fine = refined_z(doubled(e1[at_t, pl.ds(1, size_z1 + 2), gy], at_t % 4))
            fine = fine[1:1 + size_z + 2]
            low = refined_z(e1[at_t, pl.ds(2, size_z1), under, pl.ds(rows1 - 1, 1)])
            high = refined_z(e1[at_t, pl.ds(2, size_z1), over, pl.ds(0, 1)])
            for p in own:
                v0w[p] = v0b[p] + fine
                y0[2, 0, p - 1] = y0[1, 0, p - 1] + low
                y0[2, 1, p - 1] = y0[1, 1, p - 1] + high

    corrected0((1, 2, size_t1 + 1, size_t1 + 2))
    sweep0(v0w, y0.at[2], v0x, ys0.at[2], ends)
    over_t = exchange_t(2, v0x)
    corrected0(range(3, size_t1 + 1))
    sweep0(v0w, y0.at[2], v0x, ys0.at[2], inside)
    sides = exchange_sides(2, v0x, ys0.at[2], y0.at[3])
    finish(sides)
    sweep0(v0x, y0.at[3], v0s, ys0.at[3], inside, sol_ref)
    finish(over_t)
    sweep0(v0x, y0.at[3], v0s, ys0.at[3], ends, sol_ref)
    earlier = len(sent)
    over_t = exchange_t(3, v0s)
    sides = exchange_sides(3, v0s, ys0.at[3], y0.at[4])
    finish_sends(sent[:earlier])

    def residual(ts):
        for t in ts:
            slab, summed = sum0(v0s, y0.at[4], t)
            res_ref[t] = s_ref[t] + summed - (8.0 + m_ref[t]) * slab

    finish(sides)
    residual(inside)
    finish(over_t)
    residual(ends)
    finish_sends(sent[earlier:])


def coarse_full(even, odd):
    summed = even + odd
    count, rows, lanes = summed.shape
    summed = summed.reshape(count // 2, 2, rows, lanes)
    summed = summed[:, 0] + summed[:, 1]
    summed = summed + pair_swap(summed, 1, 1)
    return (summed + pair_swap(summed, 4, 2)) * 0.0625


def per_device(sizes, right_side, mass_field):
    nta, ngz, ngy = sizes
    size_t, size_z, rows, lanes = right_side.shape
    size_t1, size_z1, rows1 = size_t // 2, size_z // 2, rows // 2
    part_t, part_z, rows2 = size_t // 4, size_z // 4, rows // 4
    vmem = lambda *shape: pltpu.VMEM(shape, jnp.float32)
    dma = lambda *shape: pltpu.SemaphoreType.DMA(shape)
    padded0 = vmem(size_t + 2, size_z + 2, rows, lanes)
    padded1 = vmem(size_t1 + 4, size_z1 + 4, ngy, rows1, lanes)
    whole2 = vmem(part_t * nta, part_z * ngz, rows2 * ngy, lanes)
    packs = vmem(nta, ngz, rows2 * ngy, lanes)
    spreads, peers = 8 * ngy + ngy - 1, nta * ngz - 1
    scratch = [
        vmem(size_t, size_z, rows, lanes), padded0, padded0, padded0, padded0, padded0,
        vmem(5, 2, size_t, size_z, 1, lanes), vmem(4, 2, size_t, size_z, 1, lanes),
        vmem(max(size_t1, part_t + 2), size_z, max(rows, ngy * rows1), lanes),
        *[padded1] * 8, vmem(part_t + 2, part_z + 2, ngy * rows1, lanes),
        packs, packs, *[whole2] * 5,
        dma(4, 6), dma(4, 6), dma(2, spreads), dma(2, spreads), dma(8), dma(8),
        dma(2, peers), dma(2, peers),
        vmem(size_t, size_z, rows, lanes), vmem(size_t, size_z, rows, lanes), dma(2, size_t),
    ]
    block = jax.ShapeDtypeStruct(right_side.shape, jnp.float32)
    return pl.pallas_call(
        functools.partial(kernel, sizes),
        out_shape=(block, block),
        in_specs=[pl.BlockSpec(memory_space=pltpu.HBM)] * 2,
        out_specs=(pl.BlockSpec(memory_space=pltpu.VMEM),) * 2,
        scratch_shapes=scratch,
        compiler_params=pltpu.CompilerParams(
            collective_id=0, has_side_effects=True, vmem_limit_bytes=48 * 1024 * 1024
        ),
    )(right_side, mass_field)


def solution(mesh):
    sizes = tuple(mesh.shape[axis] for axis in ("ta", "gz", "gy"))
    spec = P("ta", "gz", "gy", None)
    return jax.shard_map(
        functools.partial(per_device, sizes),
        mesh=mesh,
        in_specs=(spec, spec),
        out_specs=(spec, spec),
        check_vma=False,
    )
```
